256 devices in a mesh: row: 8 (over x, y_hi), col: 32 (over z, y_lo, core).
Axes of the slice: x: 4, y: 4 (y_hi: 2, y_lo: 2; y = y_hi * 2 + y_lo), z: 8, core: 2. Of those that a mesh axis runs over, the one named last changes fastest.
Arguments:
- boxes: int32 [4, 65536], P(None, 'col'), may hold values from 0 to 4095, as said below
- pins: int32 [65536], P('col'), may hold values from 2 to 64
- capacity: float32 [4096, 4096], P('row', 'col'), may hold values from 4 to 12
- cell_bin: int32 [8, 65536], P('row', 'col'), may hold values from 0 to 65535
- cell_area: float32 [8, 65536], P('row', 'col'), may hold values from 1 to 10
Outputs:
- rudy: float32 [4096, 4096], P('row', 'col')
- inflation: float32 [4096, 4096], P('row', 'col')
- cell_sizes: float32 [8, 65536], P('row', 'col')
The draws below stay inside these ranges and needn't reach their ends.
Inputs may be any that keep to these rules, and one draw needn't show every extreme that they name: `boxes`: row 0 and 1 are a net's first and last bin column, row 2 and 3 its first and last bin row; first <= last, a box spans at most 512 columns and 512 rows.
All inputs are finite; a program needn't handle non-finite values.
Results may differ from the reference program's by a relative error of at most 0.0003.
Values sent between devices are 32-bit elements; how exact they have to be, the bound alone decides.
A program may use at most 64 MiB of HBM per device.

```python
import math
import jax
import jax.numpy as jnp

TILE_R = 512
TILE_C = 128
CELLS_DEV = 2048
GY = 4096
GX = 4096
NETS = 65536
SPAN_X = 512
SPAN_Y = 512
N_ROW = 8
N_COL = 32


def draw_boxes(key, part):
    keys = jax.random.split(key, 4)
    start_x = jax.random.randint(keys[0], (NETS,), 0, GX)
    width_x = jax.random.randint(keys[1], (NETS,), 1, SPAN_X + 1)
    start_y = jax.random.randint(keys[2], (NETS,), 0, GY)
    width_y = jax.random.randint(keys[3], (NETS,), 1, SPAN_Y + 1)
    end_x = jnp.minimum(start_x + width_x - 1, GX - 1)
    end_y = jnp.minimum(start_y + width_y - 1, GY - 1)
    return jnp.stack([start_x, end_x, start_y, end_y]).astype(jnp.int32)


def set_ends(values, stream_key, low, largest):
    index_at = [jax.random.randint(jax.random.fold_in(stream_key, axis), (), 0, length) for axis, length in enumerate(values.shape)]
    main_axis = values.shape.index(max(values.shape))
    next_to = index_at[:main_axis] + [(index_at[main_axis] + 1) % values.shape[main_axis]] + index_at[main_axis + 1:]
    return values.at[tuple(index_at)].set(low).at[tuple(next_to)].set(largest)


def steps_of(own_key, dims, shards, smallest, high):
    def one(axis_at, shards_of):
        draws = jax.random.uniform(jax.random.fold_in(jax.random.fold_in(own_key, 6), axis_at), (shards_of,), jnp.float32, smallest / len(shards), high / len(shards))
        return jnp.repeat(jnp.exp(draws), dims[axis_at] // shards_of).reshape((-1,) + (1,) * (len(dims) - axis_at - 1))

    loudness = one(*shards[0])
    for cut in shards[1:]:
        loudness = loudness * one(*cut)
    return loudness


def setup_inputs(seed: int = 0) -> dict:
    key_list = jax.random.split(jax.random.key(seed), 6)
    return {
        "boxes": draw_boxes(jax.random.fold_in(key_list[5], 71), 0),
        "pins": set_ends(jax.random.randint(key_list[1], (NETS,), 2, 65), jax.random.fold_in(key_list[1], 1), 2, 64).astype(jnp.int32),
        "capacity": jnp.clip(jnp.exp(math.log(12.0) - 1.0986123 * jax.random.uniform(key_list[2], (GY, GX), jnp.float32) ** steps_of(key_list[2], (GY, GX), ((0, 8), (1, 32)), -0.2, 0.2)), 4.0, 12.0),
        "cell_bin": set_ends(jax.random.randint(key_list[3], (N_ROW, N_COL * CELLS_DEV), 0, TILE_R * TILE_C), jax.random.fold_in(key_list[3], 1), 0, (TILE_R * TILE_C) - 1).astype(jnp.int32),
        "cell_area": jnp.clip(jnp.exp(math.log(10.0) - 2.3025851 * jax.random.uniform(key_list[4], (N_ROW, N_COL * CELLS_DEV), jnp.float32) ** steps_of(key_list[4], (N_ROW, N_COL * CELLS_DEV), ((0, 8), (1, 32)), -0.2, 0.2)), 1.0, 10.0),
    }


def net_weights(boxes, pins):
    span_x = (boxes[1] - boxes[0] + 1).astype(jnp.float32)
    span_y = (boxes[3] - boxes[2] + 1).astype(jnp.float32)
    weight = jnp.log(pins.astype(jnp.float32)) * (span_x + span_y) / (span_x * span_y)
    return weight.astype(jnp.bfloat16).astype(jnp.float32)


def reference(boxes, pins, capacity, cell_bin, cell_area):
    weight = net_weights(boxes, pins)
    first_x, last_x, first_y, last_y = boxes[0], boxes[1], boxes[2], boxes[3]
    corner = jnp.zeros((GY + 1, GX + 1), jnp.float32)
    corner = corner.at[first_y, first_x].add(weight)
    corner = corner.at[first_y, last_x + 1].add(-weight)
    corner = corner.at[last_y + 1, first_x].add(-weight)
    corner = corner.at[last_y + 1, last_x + 1].add(weight)
    rudy = jnp.cumsum(jnp.cumsum(corner, axis=0), axis=1)[:GY, :GX]
    excess = jnp.maximum(rudy - capacity, 0.0)
    prefix = jnp.cumsum(excess, axis=0)
    inflation = 1.0 + 2.0 * prefix / GY
    tile_row = jnp.arange(N_ROW, dtype=jnp.int32)[:, None]
    position = jnp.arange(N_COL * CELLS_DEV, dtype=jnp.int32)[None, :]
    bin_row = tile_row * TILE_R + cell_bin // TILE_C
    bin_col = (position // CELLS_DEV) * TILE_C + cell_bin % TILE_C
    grown = cell_area * inflation[bin_row, bin_col]
    cell_sizes = grown * (jnp.sum(cell_area) / jnp.sum(grown))
    return rudy, inflation, cell_sizes
```

```python
import functools

import jax
import jax.numpy as jnp
from jax import lax
from jax.experimental import pallas as pl
from jax.experimental.pallas import tpu as pltpu
from jax.sharding import PartitionSpec as P

MESH = pl.DeviceIdType.MESH
F32 = jnp.float32
BF16 = jnp.bfloat16
SLOTS = 80
HALF_SLOTS = 256
LANES = 128


def iota(shape, dim, dtype=F32):
    return lax.broadcasted_iota(jnp.int32, shape, dim).astype(dtype)


def ones_where(mask, dtype=BF16):
    return jnp.where(mask, jnp.ones((), dtype), jnp.zeros((), dtype))


def dot(a, b):
    return lax.dot_general(a, b, (((1,), (0,)), ((), ())), preferred_element_type=F32)


def dot_nt(a, b):
    return lax.dot_general(a, b, (((1,), (1,)), ((), ())), preferred_element_type=F32)


def split2(x):
    hi = x.astype(BF16)
    return hi, (x - hi.astype(F32)).astype(BF16)


def sparse_kernel(
    n_row, n_col,
    boxes_h, pins_h, cap_h, cbin_h, area_h,
    rudy_h, infl_h, sizes_h, flag_h,
    boxes, pins, cap, cbin, area, rudy, infl, sizes, flag,
    feat, hits, send, recv, onehot, early_s, early_r, mid_s, mid_r, fin_s, fin_r,
    in_sem, out_sem, a2a_ss, a2a_rs, early_ss, early_rs, mid_ss, mid_rs, fin_ss, fin_rs,
):
    row = lax.axis_index("row")
    col = lax.axis_index("col")
    tile_r, tile_c = cap.shape
    nets = pins.shape[1]
    cells = cbin.shape[1]
    chunks = nets // LANES
    half = nets // 2

    loads = [
        pltpu.make_async_copy(src, dst, in_sem.at[i])
        for i, (src, dst) in enumerate(
            ((boxes_h, boxes), (pins_h, pins), (cbin_h, cbin), (area_h, area), (cap_h, cap))
        )
    ]
    for load in loads:
        load.start()

    barrier = pltpu.get_barrier_semaphore()
    col_steps = sorted(range(1, n_col), key=lambda o: -min(o, n_col - o))
    for step in col_steps:
        pl.semaphore_signal(
            barrier, inc=1, device_id={"col": lax.rem(col + step, n_col)}, device_id_type=MESH
        )
    for step in range(1, n_row):
        pl.semaphore_signal(
            barrier, inc=1, device_id={"row": lax.rem(row + step, n_row)}, device_id_type=MESH
        )

    loads[0].wait()
    loads[1].wait()
    x0, x1, y0, y1 = (boxes[i : i + 1, :] for i in range(4))
    dx = (x1 - x0 + 1).astype(F32)
    dy = (y1 - y0 + 1).astype(F32)
    weight = jnp.log(pins[...].astype(F32)) * (dx + dy) / (dx * dy)
    weight = weight.astype(BF16).astype(F32)
    row_start = row * tile_r
    y_first = jnp.clip(y0 - row_start, 0, tile_r)
    y_end = jnp.clip(y1 + 1 - row_start, 0, tile_r)
    in_band = jnp.where(y_end > y_first, 1.0, 0.0).astype(F32)
    x_end = x1 + 1
    zero_row = jnp.zeros((1, nets), F32)
    parts = [
        (x0 & -LANES).astype(F32), (x_end & -LANES).astype(F32),
        (y_first & -256).astype(F32), (y_end & -256).astype(F32),
        weight, zero_row, zero_row, zero_row,
        (x0 & (LANES - 1)).astype(F32), (x_end & (LANES - 1)).astype(F32),
        (y_first & 255).astype(F32), (y_end & 255).astype(F32),
        zero_row, zero_row, zero_row, zero_row,
    ]
    for i, part in enumerate(parts):
        feat[i : i + 1, :] = part
    for j in range(chunks):
        hits[j : j + 1, :] = in_band[:, j * LANES : (j + 1) * LANES]
    table = feat[...].astype(BF16)
    member = hits[...].astype(BF16)
    ci, cj = iota((chunks, chunks), 0), iota((chunks, chunks), 1)
    per_half = chunks // 2
    same_half = jnp.where(ci >= per_half, 1.0, 0.0) == jnp.where(cj >= per_half, 1.0, 0.0)
    ahead = dot(ones_where((ci > cj) & same_half), member)
    before = ones_where(iota((LANES, LANES), 0) < iota((LANES, LANES), 1))
    place = dot(member, before) + dot(ahead.astype(BF16), jnp.ones((LANES, LANES), BF16))
    longest = jnp.max(place + hits[...], keepdims=True)
    place = jnp.where((hits[...] > 0.0) & (place < HALF_SLOTS), place, -1.0).astype(BF16)
    slot = iota((HALF_SLOTS, LANES), 0, BF16)
    packed = []
    for h in range(2):
        pick = jnp.concatenate(
            [
                ones_where(slot == jnp.broadcast_to(place[j : j + 1, :], slot.shape))
                for j in range(h * per_half, (h + 1) * per_half)
            ],
            axis=1,
        )
        packed.append(dot_nt(pick, table[:, h * half : (h + 1) * half]).T)
    packed = jnp.concatenate(packed, axis=1)
    listed = packed[0:8] + packed[8:16]
    band_slots = 2 * HALF_SLOTS

    tile_x = iota((n_col, band_slots), 0) * tile_c
    meets = (listed[0:1] < tile_x + tile_c) & (listed[1:2] > tile_x)
    wide = band_slots + LANES
    ti, tj = iota((band_slots, wide), 0), iota((band_slots, wide), 1)
    counted = dot(ones_where(meets), ones_where((ti < tj) | (tj >= band_slots)))
    order = counted[:, :band_slots]
    count = jnp.where(longest > HALF_SLOTS, 1e6, counted[:, band_slots:])
    odd = lax.rem(col, 2).astype(F32)
    order = jnp.where(meets, odd * (SLOTS - 1) + (1.0 - 2.0 * odd) * order, -1.0).astype(BF16)
    slot = iota((SLOTS, band_slots), 0, BF16)
    pick = jnp.concatenate(
        [
            ones_where(slot == jnp.broadcast_to(order[d : d + 1, :], slot.shape))
            for d in range(n_col)
        ],
        axis=0,
    )
    taken = dot_nt(pick, packed.astype(BF16))
    pad = jnp.zeros((LANES - SLOTS, 16), F32)
    line = lax.broadcasted_iota(jnp.int32, (8, LANES), 0)
    for d in range(n_col):
        block = jnp.concatenate([taken[d * SLOTS : (d + 1) * SLOTS], pad], axis=0).T
        send[d] = jnp.where(line == 5, count[d : d + 1, :], block[0:8] + block[8:16])

    pl.semaphore_wait(barrier, n_col - 1 + n_row - 1)
    started = []
    for step in col_steps:
        peer = lax.rem(col + step, n_col)
        copy = pltpu.make_async_remote_copy(
            src_ref=send.at[peer], dst_ref=recv.at[col],
            send_sem=a2a_ss.at[peer], recv_sem=a2a_rs.at[col],
            device_id={"col": peer}, device_id_type=MESH,
        )
        copy.start()
        started.append(copy)
    recv[col] = send[col]

    loads[2].wait()
    loads[3].wait()
    bins = cbin[...]
    bin_row = (bins // tile_c).astype(F32)
    bin_col = (bins % tile_c).astype(F32)
    for h in range(tile_r // 256):
        onehot[h * 256 : (h + 1) * 256, :] = ones_where(
            iota((256, cells), 0, BF16)
            == jnp.broadcast_to((bin_row - 256.0 * h).astype(BF16), (256, cells))
        )
    in_col = iota((tile_c, cells), 0, BF16) == jnp.broadcast_to(bin_col.astype(BF16), (tile_c, cells))
    area_hi, area_lo = split2(area[...])
    nought = jnp.zeros((), BF16)
    by_col = jnp.concatenate(
        [
            jnp.where(in_col, jnp.broadcast_to(area_hi, (tile_c, cells)), nought),
            jnp.where(in_col, jnp.broadcast_to(area_lo, (tile_c, cells)), nought),
        ],
        axis=0,
    )
    bin_area = dot_nt(onehot[...], by_col)
    bin_area = bin_area[:, :tile_c] + bin_area[:, tile_c:]
    early_s[...] = jnp.sum(bin_area, axis=0, keepdims=True)
    for step in range(1, n_row):
        peer = lax.rem(row + step, n_row)
        copy = pltpu.make_async_remote_copy(
            src_ref=early_s, dst_ref=early_r.at[row],
            send_sem=early_ss.at[peer], recv_sem=early_rs.at[row],
            device_id={"row": peer}, device_id_type=MESH,
        )
        copy.start()
        started.append(copy)
    early_r[row] = early_s[...]

    for step in reversed(col_steps):
        peer = lax.rem(col + step, n_col)
        pltpu.make_async_remote_copy(
            src_ref=send.at[peer], dst_ref=recv.at[peer],
            send_sem=a2a_ss.at[peer], recv_sem=a2a_rs.at[peer],
            device_id={"col": peer}, device_id_type=MESH,
        ).wait_recv()
    merged = []
    over = jnp.zeros((1, LANES), F32)
    for p in range(n_col // 2):
        even = recv[2 * p]
        odds = pltpu.roll(recv[2 * p + 1], LANES - SLOTS, 1)
        merged.append(even + odds)
        n_even, n_odd = even[5:6], odds[5:6]
        spilt = (n_even > SLOTS) | (n_odd > SLOTS) | (n_even + n_odd > LANES)
        over = over + jnp.where(spilt, 1.0, 0.0)
    merged = jnp.concatenate(merged, axis=1)
    total = merged.shape[1]
    shift = (col * tile_c).astype(F32)
    x_lo = jnp.clip(merged[0:1] - shift, 0.0, 1.0 * tile_c).astype(BF16)
    x_hi = jnp.clip(merged[1:2] - shift, 0.0, 1.0 * tile_c).astype(BF16)
    lane = iota((tile_c, total), 0, BF16)
    full = lambda x, n: jnp.broadcast_to(x, (n, total))
    col_weight = jnp.where(
        (lane >= full(x_lo, tile_c)) & (lane < full(x_hi, tile_c)),
        full(merged[4:5].astype(BF16), tile_c), nought,
    )
    lane = iota((256, total), 0, BF16)
    for h in range(tile_r // 256):
        y_lo = jnp.clip(merged[2:3] - 256.0 * h, 0.0, 256.0).astype(BF16)
        y_hi = jnp.clip(merged[3:4] - 256.0 * h, 0.0, 256.0).astype(BF16)
        row_hit = ones_where((lane >= full(y_lo, 256)) & (lane < full(y_hi, 256)))
        rudy[h * 256 : (h + 1) * 256, :] = dot_nt(row_hit, col_weight)
    stores = [pltpu.make_async_copy(rudy, rudy_h, out_sem.at[0])]
    stores[0].start()

    loads[4].wait()
    excess = jnp.maximum(rudy[...] - cap[...], 0.0)
    e_hi, e_lo = split2(excess)
    lower = ones_where(iota((tile_r, tile_r), 0) >= iota((tile_r, tile_r), 1))
    within = dot(lower, jnp.concatenate([e_hi, e_lo], axis=1))
    within = within[:, :tile_c] + within[:, tile_c:]
    mid_s[0:1, :] = within[tile_r - 1 : tile_r]
    mid_s[1:2, :] = jnp.sum(bin_area * within, axis=0, keepdims=True)
    mid_s[2:3, :] = over
    mid_s[3:4, :] = over
    for step in range(1, n_row):
        peer = lax.rem(row + step, n_row)
        copy = pltpu.make_async_remote_copy(
            src_ref=mid_s, dst_ref=mid_r.at[row],
            send_sem=mid_ss.at[peer], recv_sem=mid_rs.at[row],
            device_id={"row": peer}, device_id_type=MESH,
        )
        copy.start()
        started.append(copy)
    mid_r[row] = mid_s[...]
    for step in range(1, n_row):
        peer = lax.rem(row + step, n_row)
        for src, dst, ss, rs in (
            (early_s, early_r, early_ss, early_rs), (mid_s, mid_r, mid_ss, mid_rs)
        ):
            pltpu.make_async_remote_copy(
                src_ref=src, dst_ref=dst.at[peer], send_sem=ss.at[peer], recv_sem=rs.at[peer],
                device_id={"row": peer}, device_id_type=MESH,
            ).wait_recv()
    factor = 2.0 / (tile_r * n_row)
    running = jnp.zeros((1, tile_c), F32)
    carried = jnp.zeros((1, tile_c), F32)
    areas = jnp.zeros((1, tile_c), F32)
    growth = jnp.zeros((1, tile_c), F32)
    over = jnp.zeros((1, tile_c), F32)
    for r in range(n_row):
        got = mid_r[r]
        col_area = early_r[r]
        carried = jnp.where(row == r, running, carried)
        areas = areas + col_area
        growth = growth + got[1:2] + running * col_area
        running = running + got[0:1]
        over = over + got[2:3]
    fin_s[0:1, :] = areas + factor * growth
    fin_s[1:2, :] = areas
    fin_s[2:3, :] = over
    fin_s[3:4, :] = over
    for step in col_steps:
        peer = lax.rem(col + step, n_col)
        copy = pltpu.make_async_remote_copy(
            src_ref=fin_s, dst_ref=fin_r.at[col],
            send_sem=fin_ss.at[peer], recv_sem=fin_rs.at[col],
            device_id={"col": peer}, device_id_type=MESH,
        )
        copy.start()
        started.append(copy)
    fin_r[col] = fin_s[...]

    inflation = 1.0 + factor * (within + carried)
    infl[...] = inflation
    stores.append(pltpu.make_async_copy(infl, infl_h, out_sem.at[1]))
    stores[1].start()
    i_hi, i_lo = split2(inflation.T)
    looked = dot(jnp.concatenate([i_hi, i_lo], axis=0), onehot[...])
    looked = looked[:tile_c] + looked[tile_c:]
    in_col = iota((tile_c, cells), 0) == jnp.broadcast_to(bin_col, (tile_c, cells))
    looked = jnp.sum(jnp.where(in_col, looked, 0.0), axis=0, keepdims=True)
    grown = area[...] * looked

    for step in reversed(col_steps):
        peer = lax.rem(col + step, n_col)
        pltpu.make_async_remote_copy(
            src_ref=fin_s, dst_ref=fin_r.at[peer], send_sem=fin_ss.at[peer], recv_sem=fin_rs.at[peer],
            device_id={"col": peer}, device_id_type=MESH,
        ).wait_recv()
    totals = fin_r[0]
    for c in range(1, n_col):
        totals = totals + fin_r[c]
    totals = jnp.sum(totals, axis=1, keepdims=True)
    sizes[...] = grown * (totals[1:2] / totals[0:1])
    flag[...] = jnp.broadcast_to(totals[2:3], flag.shape)
    stores.append(pltpu.make_async_copy(sizes, sizes_h, out_sem.at[2]))
    stores.append(pltpu.make_async_copy(flag, flag_h, out_sem.at[3]))
    for store in stores[2:]:
        store.start()
    for copy in started:
        copy.wait_send()
    for store in stores:
        store.wait()


def sparse_program(n_row, n_col, boxes, pins, capacity, cell_bin, cell_area):
    tile_r, tile_c = capacity.shape
    nets = pins.shape[0]
    cells = cell_bin.shape[1]
    vm = pltpu.VMEM
    dma = pltpu.SemaphoreType.DMA
    anywhere = pl.BlockSpec(memory_space=pl.ANY)
    shape = jax.ShapeDtypeStruct
    return pl.pallas_call(
        functools.partial(sparse_kernel, n_row, n_col),
        name="nets_to_tiles",
        out_shape=(
            shape((tile_r, tile_c), F32), shape((tile_r, tile_c), F32),
            shape((1, cells), F32), shape((1, LANES), F32),
        ),
        in_specs=[anywhere] * 5,
        out_specs=(anywhere,) * 4,
        scratch_shapes=[
            vm((4, nets), jnp.int32), vm((1, nets), jnp.int32), vm((tile_r, tile_c), F32),
            vm((1, cells), jnp.int32), vm((1, cells), F32),
            vm((tile_r, tile_c), F32), vm((tile_r, tile_c), F32), vm((1, cells), F32),
            vm((1, LANES), F32),
            vm((16, nets), F32), vm((nets // LANES, LANES), F32),
            vm((n_col, 8, LANES), F32), vm((n_col, 8, LANES), F32),
            vm((tile_r, cells), BF16),
            vm((1, tile_c), F32), vm((n_row, 1, tile_c), F32),
            vm((4, tile_c), F32), vm((n_row, 4, tile_c), F32),
            vm((4, tile_c), F32), vm((n_col, 4, tile_c), F32),
            dma((5,)), dma((4,)),
            dma((n_col,)), dma((n_col,)), dma((n_row,)), dma((n_row,)),
            dma((n_row,)), dma((n_row,)), dma((n_col,)), dma((n_col,)),
        ],
        compiler_params=pltpu.CompilerParams(
            collective_id=0, has_side_effects=True, vmem_limit_bytes=40 * 1024 * 1024
        ),
    )(boxes, pins.reshape(1, nets), capacity, cell_bin, cell_area)


def to_everyone(shard, axis):
    peers = lax.axis_size(axis)
    return lax.all_to_all(
        jnp.broadcast_to(shard[None], (peers, *shard.shape)), axis, 0, 0, tiled=True
    )


def dense_program(boxes, pins, capacity, cell_bin, cell_area):
    tile_rows, tile_cols = capacity.shape
    table = jnp.concatenate([boxes, pins[None, :]], axis=0)
    table = to_everyone(table, "col")
    rows_here = lax.axis_index("row") * tile_rows + jnp.arange(tile_rows, dtype=jnp.int32)
    cols_here = lax.axis_index("col") * tile_cols + jnp.arange(tile_cols, dtype=jnp.int32)

    def add_block(index, acc):
        first_x, last_x, first_y, last_y, pin = table[index]
        span_x = (last_x - first_x + 1).astype(F32)
        span_y = (last_y - first_y + 1).astype(F32)
        weight = jnp.log(pin.astype(F32)) * (span_x + span_y) / (span_x * span_y)
        row_hits = (rows_here[:, None] >= first_y[None, :]) & (rows_here[:, None] <= last_y[None, :])
        col_hits = (cols_here[:, None] >= first_x[None, :]) & (cols_here[:, None] <= last_x[None, :])
        weighted = jnp.where(col_hits, weight.astype(BF16)[None, :], jnp.zeros((), BF16))
        return acc + dot_nt(row_hits.astype(BF16), weighted)

    rudy = lax.fori_loop(
        0, table.shape[0], add_block, jnp.zeros((tile_rows, tile_cols), F32)
    )
    excess = jnp.maximum(rudy - capacity, 0.0)
    ladder = jnp.arange(tile_rows, dtype=jnp.int32)
    lower = (ladder[:, None] >= ladder[None, :]).astype(F32)
    within = jnp.dot(
        lower, excess, precision=lax.Precision.HIGHEST, preferred_element_type=F32
    )
    sums = to_everyone(within[-1][None, :], "row")[:, 0]
    above = jnp.arange(sums.shape[0], dtype=jnp.int32) < lax.axis_index("row")
    carried = jnp.sum(jnp.where(above[:, None], sums, 0.0), axis=0)
    inflation = 1.0 + 2.0 * (within + carried[None, :]) / (tile_rows * lax.axis_size("row"))
    looked = jnp.take(inflation.reshape(-1), cell_bin[0], axis=0)
    grown = cell_area * looked[None, :]
    totals = jnp.stack([jnp.sum(cell_area), jnp.sum(grown)])[None, :]
    for axis in ("row", "col"):
        totals = jnp.sum(to_everyone(totals, axis), axis=0)
    cell_sizes = grown * (totals[0, 0] / totals[0, 1])
    return rudy, inflation, cell_sizes


def per_device(n_row, n_col, *args):
    rudy, inflation, cell_sizes, flag = sparse_program(n_row, n_col, *args)

    def again(state):
        held = [jnp.where(state[3][0, 0] > 0.0, x, jnp.ones((), x.dtype)) for x in args]
        return (*dense_program(*held), jnp.zeros_like(flag))

    state = lax.while_loop(
        lambda state: state[3][0, 0] > 0.0, again, (rudy, inflation, cell_sizes, flag)
    )
    return state[:3]


def solution(mesh):
    n_row, n_col = mesh.shape["row"], mesh.shape["col"]
    placed = (P(None, "col"), P("col"), P("row", "col"), P("row", "col"), P("row", "col"))
    return jax.shard_map(
        functools.partial(per_device, n_row, n_col),
        mesh=mesh,
        in_specs=placed,
        out_specs=(P("row", "col"),) * 3,
        check_vma=False,
    )
```

```python
import functools

import jax
import jax.numpy as jnp
from jax import lax
from jax.experimental import pallas as pl
from jax.experimental.pallas import tpu as pltpu
from jax.sharding import PartitionSpec as P

MESH = pl.DeviceIdType.MESH
F32 = jnp.float32
BF16 = jnp.bfloat16
SLOTS = 80
ROWS = 5
HALF_SLOTS = 256
LANES = 128


def iota(shape, dim, dtype=F32):
    return lax.broadcasted_iota(jnp.int32, shape, dim).astype(dtype)


def ones_where(mask, dtype=BF16):
    return jnp.where(mask, jnp.ones((), dtype), jnp.zeros((), dtype))


def dot(a, b):
    return lax.dot_general(a, b, (((1,), (0,)), ((), ())), preferred_element_type=F32)


def dot_nt(a, b):
    return lax.dot_general(a, b, (((1,), (1,)), ((), ())), preferred_element_type=F32)


def split2(x):
    hi = x.astype(BF16)
    return hi, (x - hi.astype(F32)).astype(BF16)


def sparse_kernel(
    n_row, n_col,
    boxes_h, pins_h, cap_h, cbin_h, area_h,
    rudy, infl, grown, totals,
    boxes, pins, cap, cbin, area,
    feat, hits, send, recv, onehot, early_s, early_r, mid_s, mid_r, fin_s, fin_r,
    in_sem, a2a_ss, a2a_rs, early_ss, early_rs, mid_ss, mid_rs, fin_ss, fin_rs,
):
    row = lax.axis_index("row")
    col = lax.axis_index("col")
    tile_r, tile_c = cap.shape
    nets = pins.shape[1]
    cells = cbin.shape[1]
    chunks = nets // LANES
    half = nets // 2

    loads = [
        pltpu.make_async_copy(src, dst, in_sem.at[i])
        for i, (src, dst) in enumerate(
            ((boxes_h, boxes), (pins_h, pins), (cbin_h, cbin), (area_h, area), (cap_h, cap))
        )
    ]
    for load in loads:
        load.start()

    barrier = pltpu.get_barrier_semaphore()
    chips = n_col // 2
    chip, core = col // 2, lax.rem(col, 2)
    far_first = sorted(range(1, chips), key=lambda o: -min(o, chips - o))
    peers = [2 * lax.rem(chip + o, chips) + k for o in far_first for k in range(2)]
    partner = 2 * chip + 1 - core
    peers.append(partner)
    for peer in peers:
        pl.semaphore_signal(barrier, inc=1, device_id={"col": peer}, device_id_type=MESH)
    for step in range(1, n_row):
        pl.semaphore_signal(
            barrier, inc=1, device_id={"row": lax.rem(row + step, n_row)}, device_id_type=MESH
        )

    loads[0].wait()
    loads[1].wait()
    x0, x1, y0, y1 = (boxes[i : i + 1, :] for i in range(4))
    dx = (x1 - x0 + 1).astype(F32)
    dy = (y1 - y0 + 1).astype(F32)
    weight = jnp.log(pins[...].astype(F32)) * (dx + dy) / (dx * dy)
    weight = weight.astype(BF16).astype(F32)
    row_start = row * tile_r
    y_first = jnp.clip(y0 - row_start, 0, tile_r)
    y_end = jnp.clip(y1 + 1 - row_start, 0, tile_r)
    in_band = jnp.where(y_end > y_first, 1.0, 0.0).astype(F32)
    x_end = x1 + 1
    zero_row = jnp.zeros((1, nets), F32)
    parts = [
        (x0 & -LANES).astype(F32), (x_end & -LANES).astype(F32),
        (y_first & -256).astype(F32), (y_end & -256).astype(F32),
        weight, zero_row, zero_row, zero_row,
        (x0 & (LANES - 1)).astype(F32), (x_end & (LANES - 1)).astype(F32),
        (y_first & 255).astype(F32), (y_end & 255).astype(F32),
        zero_row, zero_row, zero_row, zero_row,
    ]
    for i, part in enumerate(parts):
        feat[i : i + 1, :] = part
    for j in range(chunks):
        hits[j : j + 1, :] = in_band[:, j * LANES : (j + 1) * LANES]
    table = feat[...].astype(BF16)
    member = hits[...].astype(BF16)
    ci, cj = iota((chunks, chunks), 0), iota((chunks, chunks), 1)
    per_half = chunks // 2
    same_half = jnp.where(ci >= per_half, 1.0, 0.0) == jnp.where(cj >= per_half, 1.0, 0.0)
    ahead = dot(ones_where((ci > cj) & same_half), member)
    before = ones_where(iota((LANES, LANES), 0) < iota((LANES, LANES), 1))
    place = dot(member, before) + dot(ahead.astype(BF16), jnp.ones((LANES, LANES), BF16))
    longest = jnp.max(place + hits[...], keepdims=True)
    place = jnp.where((hits[...] > 0.0) & (place < HALF_SLOTS), place, -1.0).astype(BF16)
    slot = iota((HALF_SLOTS, LANES), 0, BF16)
    packed = []
    for h in range(2):
        pick = jnp.concatenate(
            [
                ones_where(slot == jnp.broadcast_to(place[j : j + 1, :], slot.shape))
                for j in range(h * per_half, (h + 1) * per_half)
            ],
            axis=1,
        )
        packed.append(dot_nt(pick, table[:, h * half : (h + 1) * half]).T)
    packed = jnp.concatenate(packed, axis=1)
    listed = packed[0:8] + packed[8:16]
    band_slots = 2 * HALF_SLOTS

    tile_x = iota((n_col, band_slots), 0) * tile_c
    meets = (listed[0:1] < tile_x + tile_c) & (listed[1:2] > tile_x)
    wide = band_slots + LANES
    ti, tj = iota((band_slots, wide), 0), iota((band_slots, wide), 1)
    counted = dot(ones_where(meets), ones_where((ti < tj) | (tj >= band_slots)))
    order = counted[:, :band_slots]
    count = jnp.where(longest > HALF_SLOTS, 1e6, counted[:, band_slots:])
    odd = core.astype(F32)
    order = jnp.where(meets, odd * (SLOTS - 1) + (1.0 - 2.0 * odd) * order, -1.0).astype(BF16)
    slot = iota((SLOTS, band_slots), 0, BF16)
    pick = jnp.concatenate(
        [
            ones_where(slot == jnp.broadcast_to(order[d : d + 1, :], slot.shape))
            for d in range(n_col)
        ],
        axis=0,
    )
    taken = dot_nt(pick, packed.astype(BF16))
    pad = jnp.zeros((LANES - SLOTS, 16), F32)
    line = lax.broadcasted_iota(jnp.int32, (8, LANES), 0)
    lane8 = lax.broadcasted_iota(jnp.int32, (8, LANES), 1)
    count_here = (line == 4) & (lane8 >= SLOTS)
    for d in range(n_col):
        block = jnp.concatenate([taken[d * SLOTS : (d + 1) * SLOTS], pad], axis=0).T
        send[d] = jnp.where(count_here, count[d : d + 1, :], block[0:8] + block[8:16])[0:ROWS]

    pl.semaphore_wait(barrier, n_col - 1 + n_row - 1)
    started = []
    for peer in peers:
        copy = pltpu.make_async_remote_copy(
            src_ref=send.at[peer], dst_ref=recv.at[col],
            send_sem=a2a_ss.at[peer], recv_sem=a2a_rs.at[col],
            device_id={"col": peer}, device_id_type=MESH,
        )
        copy.start()
        started.append(copy)
    recv[col] = send[col]

    loads[2].wait()
    loads[3].wait()
    bins = cbin[...]
    bin_row = (bins // tile_c).astype(F32)
    bin_col = (bins % tile_c).astype(F32)
    for h in range(tile_r // 256):
        onehot[h * 256 : (h + 1) * 256, :] = ones_where(
            iota((256, cells), 0, BF16)
            == jnp.broadcast_to((bin_row - 256.0 * h).astype(BF16), (256, cells))
        )
    in_col = iota((tile_c, cells), 0, BF16) == jnp.broadcast_to(bin_col.astype(BF16), (tile_c, cells))
    area_hi, area_lo = split2(area[...])
    nought = jnp.zeros((), BF16)
    by_col = jnp.concatenate(
        [
            jnp.where(in_col, jnp.broadcast_to(area_hi, (tile_c, cells)), nought),
            jnp.where(in_col, jnp.broadcast_to(area_lo, (tile_c, cells)), nought),
        ],
        axis=0,
    )
    bin_area = dot_nt(onehot[...], by_col)
    bin_area = bin_area[:, :tile_c] + bin_area[:, tile_c:]
    early_s[...] = jnp.sum(bin_area, axis=0, keepdims=True)
    for step in range(1, n_row):
        peer = lax.rem(row + step, n_row)
        copy = pltpu.make_async_remote_copy(
            src_ref=early_s, dst_ref=early_r.at[row],
            send_sem=early_ss.at[peer], recv_sem=early_rs.at[row],
            device_id={"row": peer}, device_id_type=MESH,
        )
        copy.start()
        started.append(copy)
    early_r[row] = early_s[...]

    def arrived(peer):
        pltpu.make_async_remote_copy(
            src_ref=send.at[peer], dst_ref=recv.at[peer],
            send_sem=a2a_ss.at[peer], recv_sem=a2a_rs.at[peer],
            device_id={"col": peer}, device_id_type=MESH,
        ).wait_recv()

    over = jnp.zeros((1, LANES), F32)
    near_first = [0] + far_first[::-1]
    cuts = [0, 6, 10, 14, 16] if chips == 16 else [0, chips]
    shift = (col * tile_c).astype(F32)
    lane = lax.broadcasted_iota(jnp.int32, (ROWS, LANES), 1)
    for g in range(len(cuts) - 1):
        merged = []
        for o in near_first[cuts[g] : cuts[g + 1]]:
            if o == 0:
                arrived(partner)
            else:
                arrived(2 * lax.rem(chip + o, chips))
                arrived(2 * lax.rem(chip + o, chips) + 1)
            first = 2 * lax.rem(chip + o, chips)
            even, odds = recv[first], recv[first + 1]
            n_even, n_odd = even[4:5], odds[4:5]
            spilt = (n_even > SLOTS) | (n_odd > SLOTS) | (n_even + n_odd > LANES)
            over = over + jnp.where(spilt & (lane[0:1] >= SLOTS), 1.0, 0.0)
            even = jnp.where(lane < SLOTS, even, 0.0)
            odds = jnp.where(lane < SLOTS, odds, 0.0)
            merged.append(even + pltpu.roll(odds, LANES - SLOTS, 1))
        merged = jnp.concatenate(merged, axis=1)
        total = merged.shape[1]
        full = lambda x, n: jnp.broadcast_to(x, (n, total))
        x_lo = jnp.clip(merged[0:1] - shift, 0.0, 1.0 * tile_c).astype(BF16)
        x_hi = jnp.clip(merged[1:2] - shift, 0.0, 1.0 * tile_c).astype(BF16)
        at = iota((tile_c, total), 0, BF16)
        col_weight = jnp.where(
            (at >= full(x_lo, tile_c)) & (at < full(x_hi, tile_c)),
            full(merged[4:5].astype(BF16), tile_c), nought,
        )
        at = iota((256, total), 0, BF16)
        for h in range(tile_r // 256):
            y_lo = jnp.clip(merged[2:3] - 256.0 * h, 0.0, 256.0).astype(BF16)
            y_hi = jnp.clip(merged[3:4] - 256.0 * h, 0.0, 256.0).astype(BF16)
            row_hit = ones_where((at >= full(y_lo, 256)) & (at < full(y_hi, 256)))
            part = dot_nt(row_hit, col_weight)
            rows = slice(h * 256, (h + 1) * 256)
            rudy[rows, :] = part if g == 0 else rudy[rows, :] + part

    loads[4].wait()
    excess = jnp.maximum(rudy[...] - cap[...], 0.0)
    e_hi, e_lo = split2(excess)
    lower = ones_where(iota((tile_r, tile_r), 0) >= iota((tile_r, tile_r), 1))
    within = dot(lower, jnp.concatenate([e_hi, e_lo], axis=1))
    within = within[:, :tile_c] + within[:, tile_c:]
    mid_s[0:1, :] = within[tile_r - 1 : tile_r]
    mid_s[1:2, :] = jnp.sum(bin_area * within, axis=0, keepdims=True)
    mid_s[2:3, :] = over
    for step in range(1, n_row):
        peer = lax.rem(row + step, n_row)
        copy = pltpu.make_async_remote_copy(
            src_ref=mid_s, dst_ref=mid_r.at[row],
            send_sem=mid_ss.at[peer], recv_sem=mid_rs.at[row],
            device_id={"row": peer}, device_id_type=MESH,
        )
        copy.start()
        started.append(copy)
    mid_r[row] = mid_s[...]
    for step in range(1, n_row):
        peer = lax.rem(row + step, n_row)
        for src, dst, ss, rs in (
            (early_s, early_r, early_ss, early_rs), (mid_s, mid_r, mid_ss, mid_rs)
        ):
            pltpu.make_async_remote_copy(
                src_ref=src, dst_ref=dst.at[peer], send_sem=ss.at[peer], recv_sem=rs.at[peer],
                device_id={"row": peer}, device_id_type=MESH,
            ).wait_recv()
    factor = 2.0 / (tile_r * n_row)
    running = jnp.zeros((1, tile_c), F32)
    carried = jnp.zeros((1, tile_c), F32)
    areas = jnp.zeros((1, tile_c), F32)
    growth = jnp.zeros((1, tile_c), F32)
    over = jnp.zeros((1, tile_c), F32)
    for r in range(n_row):
        got = mid_r[r]
        col_area = early_r[r]
        carried = jnp.where(row == r, running, carried)
        areas = areas + col_area
        growth = growth + got[1:2] + running * col_area
        running = running + got[0:1]
        over = over + got[2:3]
    line = lax.broadcasted_iota(jnp.int32, (8, LANES), 0)
    sums = jnp.where(line == 0, areas + factor * growth, jnp.where(line == 1, areas, over))
    sums = jnp.sum(sums, axis=1, keepdims=True)
    lane = lax.broadcasted_iota(jnp.int32, (1, LANES), 1)
    fin_s[...] = jnp.where(lane == 0, sums[0:1], jnp.where(lane == 1, sums[1:2], sums[2:3]))
    for peer in peers:
        copy = pltpu.make_async_remote_copy(
            src_ref=fin_s, dst_ref=fin_r.at[col],
            send_sem=fin_ss.at[peer], recv_sem=fin_rs.at[col],
            device_id={"col": peer}, device_id_type=MESH,
        )
        copy.start()
        started.append(copy)
    fin_r[col] = fin_s[...]

    inflation = 1.0 + factor * (within + carried)
    infl[...] = inflation
    i_hi, i_lo = split2(inflation.T)
    looked = dot(jnp.concatenate([i_hi, i_lo], axis=0), onehot[...])
    looked = looked[:tile_c] + looked[tile_c:]
    in_col = iota((tile_c, cells), 0) == jnp.broadcast_to(bin_col, (tile_c, cells))
    looked = jnp.sum(jnp.where(in_col, looked, 0.0), axis=0, keepdims=True)
    grown[...] = area[...] * looked

    for peer in reversed(peers):
        pltpu.make_async_remote_copy(
            src_ref=fin_s, dst_ref=fin_r.at[peer], send_sem=fin_ss.at[peer], recv_sem=fin_rs.at[peer],
            device_id={"col": peer}, device_id_type=MESH,
        ).wait_recv()
    parts = [fin_r[c] for c in range(n_col)]
    while len(parts) > 1:
        parts = [a + b for a, b in zip(parts[::2], parts[1::2])]
    totals[...] = parts[0]
    for copy in started:
        copy.wait_send()


def finish_kernel(rudy, infl, grown, totals, rudy_h, infl_h, sizes_h, sizes, sem):
    stores = [
        pltpu.make_async_copy(src, dst, sem.at[i])
        for i, (src, dst) in enumerate(((rudy, rudy_h), (infl, infl_h), (sizes, sizes_h)))
    ]
    stores[0].start()
    stores[1].start()
    sums = totals[...]
    sizes[...] = grown[...] * (sums[:, 1:2] / sums[:, 0:1])
    stores[2].start()
    for store in stores:
        store.wait()


def sparse_program(n_row, n_col, boxes, pins, capacity, cell_bin, cell_area):
    tile_r, tile_c = capacity.shape
    nets = pins.shape[0]
    cells = cell_bin.shape[1]
    vm = pltpu.VMEM
    dma = pltpu.SemaphoreType.DMA
    anywhere = pl.BlockSpec(memory_space=pl.ANY)
    inside = pl.BlockSpec(memory_space=pltpu.VMEM)
    shape = jax.ShapeDtypeStruct
    held = pl.pallas_call(
        functools.partial(sparse_kernel, n_row, n_col),
        name="nets_to_tiles",
        out_shape=(
            vm((tile_r, tile_c), F32), vm((tile_r, tile_c), F32),
            vm((1, cells), F32), vm((1, LANES), F32),
        ),
        in_specs=[anywhere] * 5,
        out_specs=(inside,) * 4,
        scratch_shapes=[
            vm((4, nets), jnp.int32), vm((1, nets), jnp.int32), vm((tile_r, tile_c), F32),
            vm((1, cells), jnp.int32), vm((1, cells), F32),
            vm((16, nets), F32), vm((nets // LANES, LANES), F32),
            vm((n_col, ROWS, LANES), F32), vm((n_col, ROWS, LANES), F32),
            vm((tile_r, cells), BF16),
            vm((1, tile_c), F32), vm((n_row, 1, tile_c), F32),
            vm((3, tile_c), F32), vm((n_row, 3, tile_c), F32),
            vm((1, tile_c), F32), vm((n_col, 1, tile_c), F32),
            dma((5,)),
            dma((n_col,)), dma((n_col,)), dma((n_row,)), dma((n_row,)),
            dma((n_row,)), dma((n_row,)), dma((n_col,)), dma((n_col,)),
        ],
        compiler_params=pltpu.CompilerParams(
            collective_id=0, has_side_effects=True, vmem_limit_bytes=24 * 1024 * 1024
        ),
    )(boxes, pins.reshape(1, nets), capacity, cell_bin, cell_area)
    outs = pl.pallas_call(
        finish_kernel,
        name="finish",
        out_shape=(
            shape((tile_r, tile_c), F32), shape((tile_r, tile_c), F32), shape((1, cells), F32),
        ),
        in_specs=[inside] * 4,
        out_specs=(anywhere,) * 3,
        scratch_shapes=[vm((1, cells), F32), dma((3,))],
        compiler_params=pltpu.CompilerParams(vmem_limit_bytes=4 * 1024 * 1024),
    )(*held)
    return (*outs, held[3])


def to_everyone(shard, axis):
    peers = lax.axis_size(axis)
    return lax.all_to_all(
        jnp.broadcast_to(shard[None], (peers, *shard.shape)), axis, 0, 0, tiled=True
    )


def dense_program(boxes, pins, capacity, cell_bin, cell_area):
    tile_rows, tile_cols = capacity.shape
    table = jnp.concatenate([boxes, pins[None, :]], axis=0)
    table = to_everyone(table, "col")
    rows_here = lax.axis_index("row") * tile_rows + jnp.arange(tile_rows, dtype=jnp.int32)
    cols_here = lax.axis_index("col") * tile_cols + jnp.arange(tile_cols, dtype=jnp.int32)

    def add_block(index, acc):
        first_x, last_x, first_y, last_y, pin = table[index]
        span_x = (last_x - first_x + 1).astype(F32)
        span_y = (last_y - first_y + 1).astype(F32)
        weight = jnp.log(pin.astype(F32)) * (span_x + span_y) / (span_x * span_y)
        row_hits = (rows_here[:, None] >= first_y[None, :]) & (rows_here[:, None] <= last_y[None, :])
        col_hits = (cols_here[:, None] >= first_x[None, :]) & (cols_here[:, None] <= last_x[None, :])
        weighted = jnp.where(col_hits, weight.astype(BF16)[None, :], jnp.zeros((), BF16))
        return acc + dot_nt(row_hits.astype(BF16), weighted)

    rudy = lax.fori_loop(
        0, table.shape[0], add_block, jnp.zeros((tile_rows, tile_cols), F32)
    )
    excess = jnp.maximum(rudy - capacity, 0.0)
    ladder = jnp.arange(tile_rows, dtype=jnp.int32)
    lower = (ladder[:, None] >= ladder[None, :]).astype(F32)
    within = jnp.dot(
        lower, excess, precision=lax.Precision.HIGHEST, preferred_element_type=F32
    )
    sums = to_everyone(within[-1][None, :], "row")[:, 0]
    above = jnp.arange(sums.shape[0], dtype=jnp.int32) < lax.axis_index("row")
    carried = jnp.sum(jnp.where(above[:, None], sums, 0.0), axis=0)
    inflation = 1.0 + 2.0 * (within + carried[None, :]) / (tile_rows * lax.axis_size("row"))
    looked = jnp.take(inflation.reshape(-1), cell_bin[0], axis=0)
    grown = cell_area * looked[None, :]
    totals = jnp.stack([jnp.sum(cell_area), jnp.sum(grown)])[None, :]
    for axis in ("row", "col"):
        totals = jnp.sum(to_everyone(totals, axis), axis=0)
    cell_sizes = grown * (totals[0, 0] / totals[0, 1])
    return rudy, inflation, cell_sizes


def per_device(n_row, n_col, *args):
    rudy, inflation, cell_sizes, totals = sparse_program(n_row, n_col, *args)
    flag = totals[0, 2]

    def again(state):
        held = [jnp.where(state[3] > 0.0, x, jnp.ones((), x.dtype)) for x in args]
        return (*dense_program(*held), jnp.zeros_like(flag))

    state = lax.while_loop(
        lambda state: state[3] > 0.0, again, (rudy, inflation, cell_sizes, flag)
    )
    return state[:3]


def solution(mesh):
    n_row, n_col = mesh.shape["row"], mesh.shape["col"]
    placed = (P(None, "col"), P("col"), P("row", "col"), P("row", "col"), P("row", "col"))
    return jax.shard_map(
        functools.partial(per_device, n_row, n_col),
        mesh=mesh,
        in_specs=placed,
        out_specs=(P("row", "col"),) * 3,
        check_vma=False,
    )
```

```python
import functools

import jax
import jax.numpy as jnp
from jax import lax
from jax.experimental import pallas as pl
from jax.experimental.pallas import tpu as pltpu
from jax.sharding import PartitionSpec as P

MESH = pl.DeviceIdType.MESH
F32 = jnp.float32
BF16 = jnp.bfloat16
SLOTS = 80
ROWS = 5
HALF_SLOTS = 256
LANES = 128


def iota(shape, dim, dtype=F32):
    return lax.broadcasted_iota(jnp.int32, shape, dim).astype(dtype)


def ones_where(mask, dtype=BF16):
    return jnp.where(mask, jnp.ones((), dtype), jnp.zeros((), dtype))


def dot(a, b):
    return lax.dot_general(a, b, (((1,), (0,)), ((), ())), preferred_element_type=F32)


def dot_nt(a, b):
    return lax.dot_general(a, b, (((1,), (1,)), ((), ())), preferred_element_type=F32)


def split2(x):
    hi = x.astype(BF16)
    return hi, (x - hi.astype(F32)).astype(BF16)


def sparse_kernel(
    n_row, n_col,
    boxes_h, pins_h, cap_h, cbin_h, area_h,
    rudy, infl, grown, totals,
    boxes, pins, cap, cbin, area,
    feat, hits, send, recv, onehot, early_s, early_r, mid_s, mid_r, fin_s, fin_r, fall,
    in_sem, net_sent, net_got, early_sem, mid_sem, fin_sem,
):
    row = lax.axis_index("row")
    col = lax.axis_index("col")
    tile_r, tile_c = cap.shape
    nets = pins.shape[1]
    cells = cbin.shape[1]
    chunks = nets // LANES
    half = nets // 2

    loads = [
        pltpu.make_async_copy(src, dst, in_sem.at[i])
        for i, (src, dst) in enumerate(
            ((boxes_h, boxes), (pins_h, pins), (cbin_h, cbin), (area_h, area), (cap_h, cap))
        )
    ]
    for load in loads:
        load.start()

    def await_bytes(ref, count, sem):
        some = ref.at[pl.ds(0, count)]
        pltpu.make_async_copy(some, some, sem).wait()

    def to_row(src, dst, sems):
        for step in range(1, n_row):
            pltpu.make_async_remote_copy(
                src_ref=src, dst_ref=dst.at[row], send_sem=sems.at[0], recv_sem=sems.at[1],
                device_id={"row": lax.rem(row + step, n_row)}, device_id_type=MESH,
            ).start()

    barrier = pltpu.get_barrier_semaphore()
    chips = n_col // 2
    chip, core = col // 2, lax.rem(col, 2)
    far_first = sorted(range(1, chips), key=lambda o: -min(o, chips - o))
    peers = [2 * lax.rem(chip + o, chips) + k for o in far_first for k in range(2)]
    partner = 2 * chip + 1 - core
    peers.append(partner)
    near_first = [0] + far_first[::-1]
    cuts = [0, 5, 9, 13, 16] if chips == 16 else [0, chips]
    groups = [near_first[a:b] for a, b in zip(cuts, cuts[1:])]
    group_of = {o: g for g, group in enumerate(groups) for o in group}
    steps = [o for o in far_first for k in range(2)] + [0]
    for peer in peers:
        pl.semaphore_signal(barrier, inc=1, device_id={"col": peer}, device_id_type=MESH)
    for step in range(1, n_row):
        pl.semaphore_signal(
            barrier, inc=1, device_id={"row": lax.rem(row + step, n_row)}, device_id_type=MESH
        )

    loads[0].wait()
    loads[1].wait()
    x0, x1, y0, y1 = (boxes[i : i + 1, :] for i in range(4))
    dx = (x1 - x0 + 1).astype(F32)
    dy = (y1 - y0 + 1).astype(F32)
    weight = jnp.log(pins[...].astype(F32)) * (dx + dy) / (dx * dy)
    weight = weight.astype(BF16).astype(F32)
    row_start = row * tile_r
    y_first = jnp.clip(y0 - row_start, 0, tile_r)
    y_end = jnp.clip(y1 + 1 - row_start, 0, tile_r)
    in_band = jnp.where(y_end > y_first, 1.0, 0.0).astype(F32)
    x_end = x1 + 1
    zero_row = jnp.zeros((1, nets), F32)
    parts = [
        (x0 & -LANES).astype(F32), (x_end & -LANES).astype(F32),
        (y_first & -256).astype(F32), (y_end & -256).astype(F32),
        weight, zero_row, zero_row, zero_row,
        (x0 & (LANES - 1)).astype(F32), (x_end & (LANES - 1)).astype(F32),
        (y_first & 255).astype(F32), (y_end & 255).astype(F32),
        zero_row, zero_row, zero_row, zero_row,
    ]
    for i, part in enumerate(parts):
        feat[i : i + 1, :] = part
    for j in range(chunks):
        hits[j : j + 1, :] = in_band[:, j * LANES : (j + 1) * LANES]
    table = feat[...].astype(BF16)
    member = hits[...].astype(BF16)
    ci, cj = iota((chunks, chunks), 0), iota((chunks, chunks), 1)
    per_half = chunks // 2
    same_half = jnp.where(ci >= per_half, 1.0, 0.0) == jnp.where(cj >= per_half, 1.0, 0.0)
    ahead = dot(ones_where((ci > cj) & same_half), member)
    before = ones_where(iota((LANES, LANES), 0) < iota((LANES, LANES), 1))
    place = dot(member, before) + dot(ahead.astype(BF16), jnp.ones((LANES, LANES), BF16))
    longest = jnp.max(place + hits[...], keepdims=True)
    place = jnp.where((hits[...] > 0.0) & (place < HALF_SLOTS), place, -1.0).astype(BF16)
    slot = iota((HALF_SLOTS, LANES), 0, BF16)
    packed = []
    for h in range(2):
        pick = jnp.concatenate(
            [
                ones_where(slot == jnp.broadcast_to(place[j : j + 1, :], slot.shape))
                for j in range(h * per_half, (h + 1) * per_half)
            ],
            axis=1,
        )
        packed.append(dot_nt(pick, table[:, h * half : (h + 1) * half]).T)
    packed = jnp.concatenate(packed, axis=1)
    listed = packed[0:8] + packed[8:16]
    band_slots = 2 * HALF_SLOTS

    tile_x = iota((n_col, band_slots), 0) * tile_c
    meets = (listed[0:1] < tile_x + tile_c) & (listed[1:2] > tile_x)
    wide = band_slots + LANES
    ti, tj = iota((band_slots, wide), 0), iota((band_slots, wide), 1)
    counted = dot(ones_where(meets), ones_where((ti < tj) | (tj >= band_slots)))
    order = counted[:, :band_slots]
    count = jnp.where(longest > HALF_SLOTS, 1e6, counted[:, band_slots:])
    odd = core.astype(F32)
    order = jnp.where(meets, odd * (SLOTS - 1) + (1.0 - 2.0 * odd) * order, -1.0).astype(BF16)
    slot = iota((SLOTS, band_slots), 0, BF16)
    pick = jnp.concatenate(
        [
            ones_where(slot == jnp.broadcast_to(order[d : d + 1, :], slot.shape))
            for d in range(n_col)
        ],
        axis=0,
    )
    taken = dot_nt(pick, packed.astype(BF16))
    pad = jnp.zeros((LANES - SLOTS, 16), F32)
    line = lax.broadcasted_iota(jnp.int32, (8, LANES), 0)
    lane8 = lax.broadcasted_iota(jnp.int32, (8, LANES), 1)
    count_here = (line == 4) & (lane8 >= SLOTS)
    for d in range(n_col):
        block = jnp.concatenate([taken[d * SLOTS : (d + 1) * SLOTS], pad], axis=0).T
        send[d] = jnp.where(count_here, count[d : d + 1, :], block[0:8] + block[8:16])[0:ROWS]

    pl.semaphore_wait(barrier, n_col - 1 + n_row - 1)
    for peer, o in zip(peers, steps):
        pltpu.make_async_remote_copy(
            src_ref=send.at[peer], dst_ref=recv.at[col],
            send_sem=net_sent, recv_sem=net_got.at[group_of[o]],
            device_id={"col": peer}, device_id_type=MESH,
        ).start()
    recv[col] = send[col]

    loads[2].wait()
    loads[3].wait()
    bins = cbin[...]
    bin_row = (bins // tile_c).astype(F32)
    bin_col = (bins % tile_c).astype(F32)
    for h in range(tile_r // 256):
        onehot[h * 256 : (h + 1) * 256, :] = ones_where(
            iota((256, cells), 0, BF16)
            == jnp.broadcast_to((bin_row - 256.0 * h).astype(BF16), (256, cells))
        )
    in_col = iota((tile_c, cells), 0, BF16) == jnp.broadcast_to(bin_col.astype(BF16), (tile_c, cells))
    area_hi, area_lo = split2(area[...])
    nought = jnp.zeros((), BF16)
    by_col = jnp.concatenate(
        [
            jnp.where(in_col, jnp.broadcast_to(area_hi, (tile_c, cells)), nought),
            jnp.where(in_col, jnp.broadcast_to(area_lo, (tile_c, cells)), nought),
        ],
        axis=0,
    )
    bin_area = dot_nt(onehot[...], by_col)
    bin_area = bin_area[:, :tile_c] + bin_area[:, tile_c:]
    early_s[...] = jnp.sum(bin_area, axis=0, keepdims=True)
    to_row(early_s, early_r, early_sem)
    early_r[row] = early_s[...]
    w_hi, w_lo = split2(bin_area)
    upper = ones_where(iota((tile_r, tile_r), 0) <= iota((tile_r, tile_r), 1))
    below = dot(upper, jnp.concatenate([w_hi, w_lo], axis=1))
    fall[...] = below[:, :tile_c] + below[:, tile_c:]

    over = jnp.zeros((1, LANES), F32)
    shift = (col * tile_c).astype(F32)
    lane = lax.broadcasted_iota(jnp.int32, (ROWS, LANES), 1)
    for g, group in enumerate(groups):
        merged = []
        await_bytes(recv, 2 * len(group) - (1 if g == 0 else 0), net_got.at[g])
        for o in group:
            first = 2 * lax.rem(chip + o, chips)
            even, odds = recv[first], recv[first + 1]
            n_even, n_odd = even[4:5], odds[4:5]
            spilt = (n_even > SLOTS) | (n_odd > SLOTS) | (n_even + n_odd > LANES)
            over = over + jnp.where(spilt & (lane[0:1] >= SLOTS), 1.0, 0.0)
            even = jnp.where(lane < SLOTS, even, 0.0)
            odds = jnp.where(lane < SLOTS, odds, 0.0)
            merged.append(even + pltpu.roll(odds, LANES - SLOTS, 1))
        merged = jnp.concatenate(merged, axis=1)
        total = merged.shape[1]
        full = lambda x, n: jnp.broadcast_to(x, (n, total))
        x_lo = jnp.clip(merged[0:1] - shift, 0.0, 1.0 * tile_c).astype(BF16)
        x_hi = jnp.clip(merged[1:2] - shift, 0.0, 1.0 * tile_c).astype(BF16)
        at = iota((tile_c, total), 0, BF16)
        col_weight = jnp.where(
            (at >= full(x_lo, tile_c)) & (at < full(x_hi, tile_c)),
            full(merged[4:5].astype(BF16), tile_c), nought,
        )
        at = iota((256, total), 0, BF16)
        for h in range(tile_r // 256):
            y_lo = jnp.clip(merged[2:3] - 256.0 * h, 0.0, 256.0).astype(BF16)
            y_hi = jnp.clip(merged[3:4] - 256.0 * h, 0.0, 256.0).astype(BF16)
            row_hit = ones_where((at >= full(y_lo, 256)) & (at < full(y_hi, 256)))
            part = dot_nt(row_hit, col_weight)
            rows = slice(h * 256, (h + 1) * 256)
            rudy[rows, :] = part if g == 0 else rudy[rows, :] + part

    loads[4].wait()
    excess = jnp.maximum(rudy[...] - cap[...], 0.0)
    mid_s[0:1, :] = jnp.sum(excess, axis=0, keepdims=True)
    mid_s[1:2, :] = jnp.sum(excess * fall[...], axis=0, keepdims=True) + 1e30 * over
    to_row(mid_s, mid_r, mid_sem)
    mid_r[row] = mid_s[...]
    e_hi, e_lo = split2(excess)
    lower = ones_where(iota((tile_r, tile_r), 0) >= iota((tile_r, tile_r), 1))
    within = dot(lower, jnp.concatenate([e_hi, e_lo], axis=1))
    infl[...] = within[:, :tile_c] + within[:, tile_c:]
    await_bytes(early_r, n_row - 1, early_sem.at[1])
    await_bytes(mid_r, n_row - 1, mid_sem.at[1])
    factor = 2.0 / (tile_r * n_row)
    running = jnp.zeros((1, tile_c), F32)
    carried = jnp.zeros((1, tile_c), F32)
    areas = jnp.zeros((1, tile_c), F32)
    growth = jnp.zeros((1, tile_c), F32)
    for r in range(n_row):
        got = mid_r[r]
        col_area = early_r[r]
        carried = jnp.where(row == r, running, carried)
        areas = areas + col_area
        growth = growth + got[1:2] + running * col_area
        running = running + got[0:1]
    fin_s[0:1, :] = areas + factor * growth
    fin_s[1:2, :] = areas
    for peer in peers:
        pltpu.make_async_remote_copy(
            src_ref=fin_s, dst_ref=fin_r.at[col], send_sem=fin_sem.at[0], recv_sem=fin_sem.at[1],
            device_id={"col": peer}, device_id_type=MESH,
        ).start()
    fin_r[col] = fin_s[...]

    inflation = 1.0 + factor * (infl[...] + carried)
    infl[...] = inflation
    i_hi, i_lo = split2(inflation.T)
    looked = dot(jnp.concatenate([i_hi, i_lo], axis=0), onehot[...])
    looked = looked[:tile_c] + looked[tile_c:]
    in_col = iota((tile_c, cells), 0) == jnp.broadcast_to(bin_col, (tile_c, cells))
    looked = jnp.sum(jnp.where(in_col, looked, 0.0), axis=0, keepdims=True)
    grown[...] = area[...] * looked

    await_bytes(send, n_col - 1, net_sent)
    await_bytes(early_r, n_row - 1, early_sem.at[0])
    await_bytes(mid_r, n_row - 1, mid_sem.at[0])
    await_bytes(fin_r, n_col - 1, fin_sem.at[1])
    parts = [fin_r[c] for c in range(n_col)]
    while len(parts) > 1:
        parts = [a + b for a, b in zip(parts[::2], parts[1::2])]
    totals[...] = parts[0]
    await_bytes(fin_r, n_col - 1, fin_sem.at[0])


def finish_kernel(rudy, infl, grown, totals, rudy_h, infl_h, sizes_h, flag_h, sizes, flag, sem):
    stores = [
        pltpu.make_async_copy(src, dst, sem.at[i])
        for i, (src, dst) in enumerate(
            ((rudy, rudy_h), (infl, infl_h), (sizes, sizes_h), (flag, flag_h))
        )
    ]
    stores[0].start()
    stores[1].start()
    sums = jnp.sum(totals[...], axis=1, keepdims=True)
    flag[...] = jnp.broadcast_to(sums[0:1], flag.shape)
    stores[3].start()
    sizes[...] = grown[...] * (sums[1:2] / sums[0:1])
    stores[2].start()
    for store in stores:
        store.wait()


def sparse_program(n_row, n_col, boxes, pins, capacity, cell_bin, cell_area):
    tile_r, tile_c = capacity.shape
    nets = pins.shape[0]
    cells = cell_bin.shape[1]
    vm = pltpu.VMEM
    dma = pltpu.SemaphoreType.DMA
    anywhere = pl.BlockSpec(memory_space=pl.ANY)
    inside = pl.BlockSpec(memory_space=pltpu.VMEM)
    shape = jax.ShapeDtypeStruct
    held = pl.pallas_call(
        functools.partial(sparse_kernel, n_row, n_col),
        name="nets_to_tiles",
        out_shape=(
            vm((tile_r, tile_c), F32), vm((tile_r, tile_c), F32),
            vm((1, cells), F32), vm((2, LANES), F32),
        ),
        in_specs=[anywhere] * 5,
        out_specs=(inside,) * 4,
        scratch_shapes=[
            vm((4, nets), jnp.int32), vm((1, nets), jnp.int32), vm((tile_r, tile_c), F32),
            vm((1, cells), jnp.int32), vm((1, cells), F32),
            vm((16, nets), F32), vm((nets // LANES, LANES), F32),
            vm((n_col, ROWS, LANES), F32), vm((n_col, ROWS, LANES), F32),
            vm((tile_r, cells), BF16),
            vm((1, tile_c), F32), vm((n_row, 1, tile_c), F32),
            vm((2, tile_c), F32), vm((n_row, 2, tile_c), F32),
            vm((2, tile_c), F32), vm((n_col, 2, tile_c), F32),
            vm((tile_r, tile_c), F32),
            dma((5,)), dma(()), dma((4,)), dma((2,)), dma((2,)), dma((2,)),
        ],
        compiler_params=pltpu.CompilerParams(
            collective_id=0, has_side_effects=True, vmem_limit_bytes=24 * 1024 * 1024
        ),
    )(boxes, pins.reshape(1, nets), capacity, cell_bin, cell_area)
    return pl.pallas_call(
        finish_kernel,
        name="finish",
        out_shape=(
            shape((tile_r, tile_c), F32), shape((tile_r, tile_c), F32), shape((1, cells), F32),
            shape((1, LANES), F32),
        ),
        in_specs=[inside] * 4,
        out_specs=(anywhere,) * 4,
        scratch_shapes=[vm((1, cells), F32), vm((1, LANES), F32), dma((4,))],
        compiler_params=pltpu.CompilerParams(vmem_limit_bytes=4 * 1024 * 1024),
    )(*held)


def to_everyone(shard, axis):
    peers = lax.axis_size(axis)
    return lax.all_to_all(
        jnp.broadcast_to(shard[None], (peers, *shard.shape)), axis, 0, 0, tiled=True
    )


def dense_program(boxes, pins, capacity, cell_bin, cell_area):
    tile_rows, tile_cols = capacity.shape
    table = jnp.concatenate([boxes, pins[None, :]], axis=0)
    table = to_everyone(table, "col")
    rows_here = lax.axis_index("row") * tile_rows + jnp.arange(tile_rows, dtype=jnp.int32)
    cols_here = lax.axis_index("col") * tile_cols + jnp.arange(tile_cols, dtype=jnp.int32)

    def add_block(index, acc):
        first_x, last_x, first_y, last_y, pin = table[index]
        span_x = (last_x - first_x + 1).astype(F32)
        span_y = (last_y - first_y + 1).astype(F32)
        weight = jnp.log(pin.astype(F32)) * (span_x + span_y) / (span_x * span_y)
        row_hits = (rows_here[:, None] >= first_y[None, :]) & (rows_here[:, None] <= last_y[None, :])
        col_hits = (cols_here[:, None] >= first_x[None, :]) & (cols_here[:, None] <= last_x[None, :])
        weighted = jnp.where(col_hits, weight.astype(BF16)[None, :], jnp.zeros((), BF16))
        return acc + dot_nt(row_hits.astype(BF16), weighted)

    rudy = lax.fori_loop(
        0, table.shape[0], add_block, jnp.zeros((tile_rows, tile_cols), F32)
    )
    excess = jnp.maximum(rudy - capacity, 0.0)
    ladder = jnp.arange(tile_rows, dtype=jnp.int32)
    lower = (ladder[:, None] >= ladder[None, :]).astype(F32)
    within = jnp.dot(
        lower, excess, precision=lax.Precision.HIGHEST, preferred_element_type=F32
    )
    sums = to_everyone(within[-1][None, :], "row")[:, 0]
    above = jnp.arange(sums.shape[0], dtype=jnp.int32) < lax.axis_index("row")
    carried = jnp.sum(jnp.where(above[:, None], sums, 0.0), axis=0)
    inflation = 1.0 + 2.0 * (within + carried[None, :]) / (tile_rows * lax.axis_size("row"))
    looked = jnp.take(inflation.reshape(-1), cell_bin[0], axis=0)
    grown = cell_area * looked[None, :]
    totals = jnp.stack([jnp.sum(cell_area), jnp.sum(grown)])[None, :]
    for axis in ("row", "col"):
        totals = jnp.sum(to_everyone(totals, axis), axis=0)
    cell_sizes = grown * (totals[0, 0] / totals[0, 1])
    return rudy, inflation, cell_sizes


def per_device(n_row, n_col, *args):
    rudy, inflation, cell_sizes, flag = sparse_program(n_row, n_col, *args)

    def again(state):
        held = [jnp.where(state[3][0, 0] > 1e20, x, jnp.ones((), x.dtype)) for x in args]
        return (*dense_program(*held), jnp.zeros_like(flag))

    state = lax.while_loop(
        lambda state: state[3][0, 0] > 1e20, again, (rudy, inflation, cell_sizes, flag)
    )
    return state[:3]


def solution(mesh):
    n_row, n_col = mesh.shape["row"], mesh.shape["col"]
    placed = (P(None, "col"), P("col"), P("row", "col"), P("row", "col"), P("row", "col"))
    return jax.shard_map(
        functools.partial(per_device, n_row, n_col),
        mesh=mesh,
        in_specs=placed,
        out_specs=(P("row", "col"),) * 3,
        check_vma=False,
    )
```

```python
import functools

import jax
import jax.numpy as jnp
from jax import lax
from jax.experimental import pallas as pl
from jax.experimental.pallas import tpu as pltpu
from jax.sharding import PartitionSpec as P

MESH = pl.DeviceIdType.MESH
F32 = jnp.float32
BF16 = jnp.bfloat16
SLOTS = 80
ROWS = 5
PIECES = 4
HALF_SLOTS = 256
LANES = 128


def iota(shape, dim, dtype=F32):
    return lax.broadcasted_iota(jnp.int32, shape, dim).astype(dtype)


def ones_where(mask, dtype=BF16):
    return jnp.where(mask, jnp.ones((), dtype), jnp.zeros((), dtype))


def dot(a, b):
    return lax.dot_general(a, b, (((1,), (0,)), ((), ())), preferred_element_type=F32)


def dot_nt(a, b):
    return lax.dot_general(a, b, (((1,), (1,)), ((), ())), preferred_element_type=F32)


def split2(x):
    hi = x.astype(BF16)
    return hi, (x - hi.astype(F32)).astype(BF16)


def sparse_kernel(
    n_row, n_col,
    boxes_h, pins_h, cap_h, cbin_h, area_h,
    rudy, infl, grown, totals,
    boxes, pins, cap, cbin, area,
    feat, hits, send, recv, onehot, early_s, early_r, mid_s, mid_r, fin_s, fin_r, fall, kept,
    in_sem, net_sent, net_got, early_sem, mid_sem, fin_sem,
):
    row = lax.axis_index("row")
    col = lax.axis_index("col")
    tile_r, tile_c = cap.shape
    nets = pins.shape[1]
    cells = cbin.shape[1]
    chunks = nets // LANES
    half = nets // 2

    loads = [
        pltpu.make_async_copy(src, dst, in_sem.at[i])
        for i, (src, dst) in enumerate(
            ((boxes_h, boxes), (pins_h, pins), (cbin_h, cbin), (area_h, area), (cap_h, cap))
        )
    ]
    for load in loads:
        load.start()

    def await_bytes(ref, count, sem):
        some = ref.at[pl.ds(0, count)]
        pltpu.make_async_copy(some, some, sem).wait()

    quad, place4 = col // 4, lax.rem(col, 4)
    member = row * 4 + place4
    plane = [
        (dr, {"row": lax.rem(row + dr, n_row), "col": 4 * quad + lax.rem(place4 + dq, 4)})
        for dr in sorted(range(n_row), key=lambda d: -min(d, n_row - d) - 2 * (d % 2))
        for dq in range(4)
        if dr or dq
    ]

    def to_plane(src, dst, sems):
        for _, peer in plane:
            pltpu.make_async_remote_copy(
                src_ref=src, dst_ref=dst.at[member], send_sem=sems.at[0], recv_sem=sems.at[1],
                device_id=peer, device_id_type=MESH,
            ).start()

    barrier = pltpu.get_barrier_semaphore()
    chips = n_col // 2
    chip, core = col // 2, lax.rem(col, 2)
    far_first = sorted(range(1, chips), key=lambda o: -min(o, chips - o))
    peers = [2 * lax.rem(chip + o, chips) + k for o in far_first for k in range(2)]
    partner = 2 * chip + 1 - core
    peers.append(partner)
    near_first = [0] + far_first[::-1]
    cuts = [0, 5, 9, 13, 16] if chips == 16 else [0, chips]
    groups = [near_first[a:b] for a, b in zip(cuts, cuts[1:])]
    group_of = {o: g for g, group in enumerate(groups) for o in group}
    steps = [o for o in far_first for k in range(2)] + [0]
    for peer in peers:
        pl.semaphore_signal(barrier, inc=1, device_id={"col": peer}, device_id_type=MESH)
    for dr, peer in plane:
        if dr:
            pl.semaphore_signal(barrier, inc=1, device_id=peer, device_id_type=MESH)

    loads[0].wait()
    loads[1].wait()
    x0, x1, y0, y1 = (boxes[i : i + 1, :] for i in range(4))
    dx = (x1 - x0 + 1).astype(F32)
    dy = (y1 - y0 + 1).astype(F32)
    weight = jnp.log(pins[...].astype(F32)) * (dx + dy) / (dx * dy)
    weight = weight.astype(BF16).astype(F32)
    row_start = row * tile_r
    y_first = jnp.clip(y0 - row_start, 0, tile_r)
    y_end = jnp.clip(y1 + 1 - row_start, 0, tile_r)
    in_band = jnp.where(y_end > y_first, 1.0, 0.0).astype(F32)
    x_end = x1 + 1
    zero_row = jnp.zeros((1, nets), F32)
    parts = [
        (x0 & -LANES).astype(F32), (x_end & -LANES).astype(F32),
        (y_first & -256).astype(F32), (y_end & -256).astype(F32),
        weight, zero_row, zero_row, zero_row,
        (x0 & (LANES - 1)).astype(F32), (x_end & (LANES - 1)).astype(F32),
        (y_first & 255).astype(F32), (y_end & 255).astype(F32),
        zero_row, zero_row, zero_row, zero_row,
    ]
    for i, part in enumerate(parts):
        feat[i : i + 1, :] = part
    for j in range(chunks):
        hits[j : j + 1, :] = in_band[:, j * LANES : (j + 1) * LANES]
    table = feat[...].astype(BF16)
    marks = hits[...].astype(BF16)
    ci, cj = iota((chunks, chunks), 0), iota((chunks, chunks), 1)
    per_half = chunks // 2
    same_half = jnp.where(ci >= per_half, 1.0, 0.0) == jnp.where(cj >= per_half, 1.0, 0.0)
    ahead = dot(ones_where((ci > cj) & same_half), marks)
    before = ones_where(iota((LANES, LANES), 0) < iota((LANES, LANES), 1))
    place = dot(marks, before) + dot(ahead.astype(BF16), jnp.ones((LANES, LANES), BF16))
    longest = jnp.max(place + hits[...], keepdims=True)
    place = jnp.where((hits[...] > 0.0) & (place < HALF_SLOTS), place, -1.0).astype(BF16)
    slot = iota((HALF_SLOTS, LANES), 0, BF16)
    packed = []
    for h in range(2):
        pick = jnp.concatenate(
            [
                ones_where(slot == jnp.broadcast_to(place[j : j + 1, :], slot.shape))
                for j in range(h * per_half, (h + 1) * per_half)
            ],
            axis=1,
        )
        packed.append(dot_nt(pick, table[:, h * half : (h + 1) * half]).T)
    packed = jnp.concatenate(packed, axis=1)
    listed = packed[0:8] + packed[8:16]
    band_slots = 2 * HALF_SLOTS

    tile_x = iota((n_col, band_slots), 0) * tile_c
    meets = (listed[0:1] < tile_x + tile_c) & (listed[1:2] > tile_x)
    wide = band_slots + LANES
    ti, tj = iota((band_slots, wide), 0), iota((band_slots, wide), 1)
    counted = dot(ones_where(meets), ones_where((ti < tj) | (tj >= band_slots)))
    order = counted[:, :band_slots]
    count = jnp.where(longest > HALF_SLOTS, 1e6, counted[:, band_slots:])
    odd = core.astype(F32)
    order = jnp.where(meets, odd * (SLOTS - 1) + (1.0 - 2.0 * odd) * order, -1.0).astype(BF16)
    slot = iota((SLOTS, band_slots), 0, BF16)
    pick = jnp.concatenate(
        [
            ones_where(slot == jnp.broadcast_to(order[d : d + 1, :], slot.shape))
            for d in range(n_col)
        ],
        axis=0,
    )
    taken = dot_nt(pick, packed.astype(BF16))
    pad = jnp.zeros((LANES - SLOTS, 16), F32)
    line = lax.broadcasted_iota(jnp.int32, (8, LANES), 0)
    lane8 = lax.broadcasted_iota(jnp.int32, (8, LANES), 1)
    count_here = (line == 4) & (lane8 >= SLOTS)
    for d in range(n_col):
        block = jnp.concatenate([taken[d * SLOTS : (d + 1) * SLOTS], pad], axis=0).T
        send[d] = jnp.where(count_here, count[d : d + 1, :], block[0:8] + block[8:16])[0:ROWS]

    pl.semaphore_wait(barrier, n_col - 1 + 4 * (n_row - 1))
    for peer, o in zip(peers, steps):
        pltpu.make_async_remote_copy(
            src_ref=send.at[peer], dst_ref=recv.at[col],
            send_sem=net_sent, recv_sem=net_got.at[group_of[o]],
            device_id={"col": peer}, device_id_type=MESH,
        ).start()
    recv[col] = send[col]

    loads[2].wait()
    loads[3].wait()
    bins = cbin[...]
    bin_row = (bins // tile_c).astype(F32)
    bin_col = (bins % tile_c).astype(F32)
    for h in range(tile_r // 256):
        onehot[h * 256 : (h + 1) * 256, :] = ones_where(
            iota((256, cells), 0, BF16)
            == jnp.broadcast_to((bin_row - 256.0 * h).astype(BF16), (256, cells))
        )
    in_col = iota((tile_c, cells), 0, BF16) == jnp.broadcast_to(bin_col.astype(BF16), (tile_c, cells))
    area_hi, area_lo = split2(area[...])
    nought = jnp.zeros((), BF16)
    by_col = jnp.concatenate(
        [
            jnp.where(in_col, jnp.broadcast_to(area_hi, (tile_c, cells)), nought),
            jnp.where(in_col, jnp.broadcast_to(area_lo, (tile_c, cells)), nought),
        ],
        axis=0,
    )
    bin_area = dot_nt(onehot[...], by_col)
    bin_area = bin_area[:, :tile_c] + bin_area[:, tile_c:]
    early_s[...] = jnp.sum(bin_area, axis=0, keepdims=True)
    to_plane(early_s, early_r, early_sem)
    early_r[member] = early_s[...]
    w_hi, w_lo = split2(bin_area)
    upper = ones_where(iota((tile_r, tile_r), 0) <= iota((tile_r, tile_r), 1))
    below = dot(upper, jnp.concatenate([w_hi, w_lo], axis=1))
    fall[...] = below[:, :tile_c] + below[:, tile_c:]

    loads[4].wait()
    await_bytes(early_r, 4 * n_row - 1, early_sem.at[1])
    factor = 2.0 / (tile_r * n_row)
    areas_below = jnp.zeros((1, tile_c), F32)
    areas = jnp.zeros((1, tile_c), F32)
    for r in range(n_row):
        column = early_r[4 * r + place4]
        areas_below = areas_below + jnp.where(r > row, column, 0.0)
        for q in range(4):
            areas = areas + early_r[4 * r + q]
    kept[0:1, :] = areas_below
    kept[1:2, :] = areas
    over = jnp.zeros((1, LANES), F32)
    shift = (col * tile_c).astype(F32)
    lane = lax.broadcasted_iota(jnp.int32, (ROWS, LANES), 1)
    for g, group in enumerate(groups):
        merged = []
        await_bytes(recv, 2 * len(group) - (1 if g == 0 else 0), net_got.at[g])
        for o in group:
            first = 2 * lax.rem(chip + o, chips)
            even, odds = recv[first], recv[first + 1]
            n_even, n_odd = even[4:5], odds[4:5]
            spilt = (n_even > SLOTS) | (n_odd > SLOTS) | (n_even + n_odd > LANES)
            over = over + jnp.where(spilt & (lane[0:1] >= SLOTS), 1.0, 0.0)
            even = jnp.where(lane < SLOTS, even, 0.0)
            odds = jnp.where(lane < SLOTS, odds, 0.0)
            merged.append(even + pltpu.roll(odds, LANES - SLOTS, 1))
        merged = jnp.concatenate(merged, axis=1)
        total = merged.shape[1]
        full = lambda x, n: jnp.broadcast_to(x, (n, total))
        x_lo = jnp.clip(merged[0:1] - shift, 0.0, 1.0 * tile_c).astype(BF16)
        x_hi = jnp.clip(merged[1:2] - shift, 0.0, 1.0 * tile_c).astype(BF16)
        at = iota((tile_c, total), 0, BF16)
        col_weight = jnp.where(
            (at >= full(x_lo, tile_c)) & (at < full(x_hi, tile_c)),
            full(merged[4:5].astype(BF16), tile_c), nought,
        )
        at = iota((256, total), 0, BF16)
        for h in range(tile_r // 256):
            y_lo = jnp.clip(merged[2:3] - 256.0 * h, 0.0, 256.0).astype(BF16)
            y_hi = jnp.clip(merged[3:4] - 256.0 * h, 0.0, 256.0).astype(BF16)
            row_hit = ones_where((at >= full(y_lo, 256)) & (at < full(y_hi, 256)))
            part = dot_nt(row_hit, col_weight)
            rows = slice(h * 256, (h + 1) * 256)
            rudy[rows, :] = part if g == 0 else rudy[rows, :] + part

    excess = jnp.maximum(rudy[...] - cap[...], 0.0)
    column = jnp.sum(excess, axis=0, keepdims=True)
    mid_s[0:1, :] = column
    mid_s[1:2, :] = (
        jnp.sum(excess * fall[...], axis=0, keepdims=True) + column * kept[0:1, :] + 1e30 * over
    )
    to_plane(mid_s, mid_r, mid_sem)
    mid_r[member] = mid_s[...]
    e_hi, e_lo = split2(excess)
    lower = ones_where(iota((tile_r, tile_r), 0) >= iota((tile_r, tile_r), 1))
    within = dot(lower, jnp.concatenate([e_hi, e_lo], axis=1))
    infl[...] = within[:, :tile_c] + within[:, tile_c:]
    await_bytes(mid_r, 4 * n_row - 1, mid_sem.at[1])
    parts = [mid_r[m] for m in range(4 * n_row)]
    while len(parts) > 1:
        parts = [a + b for a, b in zip(parts[::2], parts[1::2])]
    fin_s[0:1, :] = kept[1:2, :] + factor * parts[0][1:2]
    fin_s[1:2, :] = kept[1:2, :]
    quads = n_col // 4
    for dz in sorted(range(1, quads), key=lambda d: -min(d, quads - d)):
        pltpu.make_async_remote_copy(
            src_ref=fin_s, dst_ref=fin_r.at[quad], send_sem=fin_sem.at[0], recv_sem=fin_sem.at[1],
            device_id={"col": 4 * lax.rem(quad + dz, quads) + place4}, device_id_type=MESH,
        ).start()
    fin_r[quad] = fin_s[...]
    carried = jnp.zeros((1, tile_c), F32)
    for r in range(n_row):
        carried = carried + jnp.where(r < row, mid_r[4 * r + place4][0:1], 0.0)

    inflation = 1.0 + factor * (infl[...] + carried)
    infl[...] = inflation
    i_hi, i_lo = split2(inflation.T)
    looked = dot(jnp.concatenate([i_hi, i_lo], axis=0), onehot[...])
    looked = looked[:tile_c] + looked[tile_c:]
    in_col = iota((tile_c, cells), 0) == jnp.broadcast_to(bin_col, (tile_c, cells))
    looked = jnp.sum(jnp.where(in_col, looked, 0.0), axis=0, keepdims=True)
    grown[...] = area[...] * looked

    await_bytes(send, n_col - 1, net_sent)
    await_bytes(early_r, 4 * n_row - 1, early_sem.at[0])
    await_bytes(mid_r, 4 * n_row - 1, mid_sem.at[0])
    await_bytes(fin_r, quads - 1, fin_sem.at[1])
    parts = [fin_r[c] for c in range(quads)]
    while len(parts) > 1:
        parts = [a + b for a, b in zip(parts[::2], parts[1::2])]
    totals[...] = parts[0]
    await_bytes(fin_r, quads - 1, fin_sem.at[0])


def finish_kernel(rudy, infl, grown, totals, rudy_h, infl_h, sizes_h, flag_h, sizes, flag, sem):
    rows = rudy.shape[0] // PIECES
    stores = []
    for src, dst, done in ((rudy, rudy_h, sem.at[0]), (infl, infl_h, sem.at[1])):
        for i in range(PIECES):
            piece = pl.ds(i * rows, rows)
            pltpu.make_async_copy(src.at[piece], dst.at[piece], done).start()
        stores.append(pltpu.make_async_copy(src, dst, done))
    stores.append(pltpu.make_async_copy(sizes, sizes_h, sem.at[2]))
    stores.append(pltpu.make_async_copy(flag, flag_h, sem.at[3]))
    sums = jnp.sum(totals[...], axis=1, keepdims=True)
    flag[...] = jnp.broadcast_to(sums[0:1], flag.shape)
    stores[3].start()
    sizes[...] = grown[...] * (sums[1:2] / sums[0:1])
    stores[2].start()
    for store in stores:
        store.wait()


def sparse_program(n_row, n_col, boxes, pins, capacity, cell_bin, cell_area):
    tile_r, tile_c = capacity.shape
    nets = pins.shape[0]
    cells = cell_bin.shape[1]
    vm = pltpu.VMEM
    dma = pltpu.SemaphoreType.DMA
    anywhere = pl.BlockSpec(memory_space=pl.ANY)
    inside = pl.BlockSpec(memory_space=pltpu.VMEM)
    shape = jax.ShapeDtypeStruct
    held = pl.pallas_call(
        functools.partial(sparse_kernel, n_row, n_col),
        name="nets_to_tiles",
        out_shape=(
            vm((tile_r, tile_c), F32), vm((tile_r, tile_c), F32),
            vm((1, cells), F32), vm((2, LANES), F32),
        ),
        in_specs=[anywhere] * 5,
        out_specs=(inside,) * 4,
        scratch_shapes=[
            vm((4, nets), jnp.int32), vm((1, nets), jnp.int32), vm((tile_r, tile_c), F32),
            vm((1, cells), jnp.int32), vm((1, cells), F32),
            vm((16, nets), F32), vm((nets // LANES, LANES), F32),
            vm((n_col, ROWS, LANES), F32), vm((n_col, ROWS, LANES), F32),
            vm((tile_r, cells), BF16),
            vm((1, tile_c), F32), vm((4 * n_row, 1, tile_c), F32),
            vm((2, tile_c), F32), vm((4 * n_row, 2, tile_c), F32),
            vm((2, tile_c), F32), vm((n_col // 4, 2, tile_c), F32),
            vm((tile_r, tile_c), F32), vm((2, tile_c), F32),
            dma((5,)), dma(()), dma((4,)), dma((2,)), dma((2,)), dma((2,)),
        ],
        compiler_params=pltpu.CompilerParams(
            collective_id=0, has_side_effects=True, vmem_limit_bytes=24 * 1024 * 1024
        ),
    )(boxes, pins.reshape(1, nets), capacity, cell_bin, cell_area)
    return pl.pallas_call(
        finish_kernel,
        name="finish",
        out_shape=(
            shape((tile_r, tile_c), F32), shape((tile_r, tile_c), F32), shape((1, cells), F32),
            shape((1, LANES), F32),
        ),
        in_specs=[inside] * 4,
        out_specs=(anywhere,) * 4,
        scratch_shapes=[vm((1, cells), F32), vm((1, LANES), F32), dma((4,))],
        compiler_params=pltpu.CompilerParams(vmem_limit_bytes=4 * 1024 * 1024),
    )(*held)


def to_everyone(shard, axis):
    peers = lax.axis_size(axis)
    return lax.all_to_all(
        jnp.broadcast_to(shard[None], (peers, *shard.shape)), axis, 0, 0, tiled=True
    )


def dense_program(boxes, pins, capacity, cell_bin, cell_area):
    tile_rows, tile_cols = capacity.shape
    table = jnp.concatenate([boxes, pins[None, :]], axis=0)
    table = to_everyone(table, "col")
    rows_here = lax.axis_index("row") * tile_rows + jnp.arange(tile_rows, dtype=jnp.int32)
    cols_here = lax.axis_index("col") * tile_cols + jnp.arange(tile_cols, dtype=jnp.int32)

    def add_block(index, acc):
        first_x, last_x, first_y, last_y, pin = table[index]
        span_x = (last_x - first_x + 1).astype(F32)
        span_y = (last_y - first_y + 1).astype(F32)
        weight = jnp.log(pin.astype(F32)) * (span_x + span_y) / (span_x * span_y)
        row_hits = (rows_here[:, None] >= first_y[None, :]) & (rows_here[:, None] <= last_y[None, :])
        col_hits = (cols_here[:, None] >= first_x[None, :]) & (cols_here[:, None] <= last_x[None, :])
        weighted = jnp.where(col_hits, weight.astype(BF16)[None, :], jnp.zeros((), BF16))
        return acc + dot_nt(row_hits.astype(BF16), weighted)

    rudy = lax.fori_loop(
        0, table.shape[0], add_block, jnp.zeros((tile_rows, tile_cols), F32)
    )
    excess = jnp.maximum(rudy - capacity, 0.0)
    ladder = jnp.arange(tile_rows, dtype=jnp.int32)
    lower = (ladder[:, None] >= ladder[None, :]).astype(F32)
    within = jnp.dot(
        lower, excess, precision=lax.Precision.HIGHEST, preferred_element_type=F32
    )
    sums = to_everyone(within[-1][None, :], "row")[:, 0]
    above = jnp.arange(sums.shape[0], dtype=jnp.int32) < lax.axis_index("row")
    carried = jnp.sum(jnp.where(above[:, None], sums, 0.0), axis=0)
    inflation = 1.0 + 2.0 * (within + carried[None, :]) / (tile_rows * lax.axis_size("row"))
    looked = jnp.take(inflation.reshape(-1), cell_bin[0], axis=0)
    grown = cell_area * looked[None, :]
    totals = jnp.stack([jnp.sum(cell_area), jnp.sum(grown)])[None, :]
    for axis in ("row", "col"):
        totals = jnp.sum(to_everyone(totals, axis), axis=0)
    cell_sizes = grown * (totals[0, 0] / totals[0, 1])
    return rudy, inflation, cell_sizes


def per_device(n_row, n_col, *args):
    rudy, inflation, cell_sizes, flag = sparse_program(n_row, n_col, *args)

    def again(state):
        held = [jnp.where(state[3][0, 0] > 1e20, x, jnp.ones((), x.dtype)) for x in args]
        return (*dense_program(*held), jnp.zeros_like(flag))

    state = lax.while_loop(
        lambda state: state[3][0, 0] > 1e20, again, (rudy, inflation, cell_sizes, flag)
    )
    return state[:3]


def solution(mesh):
    n_row, n_col = mesh.shape["row"], mesh.shape["col"]
    placed = (P(None, "col"), P("col"), P("row", "col"), P("row", "col"), P("row", "col"))
    return jax.shard_map(
        functools.partial(per_device, n_row, n_col),
        mesh=mesh,
        in_specs=placed,
        out_specs=(P("row", "col"),) * 3,
        check_vma=False,
    )
```

```python
import functools

import jax
import jax.numpy as jnp
from jax import lax
from jax.experimental import pallas as pl
from jax.experimental.pallas import tpu as pltpu
from jax.sharding import PartitionSpec as P

MESH = pl.DeviceIdType.MESH
F32 = jnp.float32
BF16 = jnp.bfloat16
SLOTS = 80
ROWS = 5
PIECES = 4
HALF_SLOTS = 256
LANES = 128


def iota(shape, dim, dtype=F32):
    return lax.broadcasted_iota(jnp.int32, shape, dim).astype(dtype)


def ones_where(mask, dtype=BF16):
    return jnp.where(mask, jnp.ones((), dtype), jnp.zeros((), dtype))


def dot(a, b):
    return lax.dot_general(a, b, (((1,), (0,)), ((), ())), preferred_element_type=F32)


def dot_nt(a, b):
    return lax.dot_general(a, b, (((1,), (1,)), ((), ())), preferred_element_type=F32)


def split2(x):
    hi = x.astype(BF16)
    return hi, (x - hi.astype(F32)).astype(BF16)


def sparse_kernel(
    n_row, n_col,
    boxes_h, pins_h, cap_h, cbin_h, area_h,
    rudy, infl, grown, totals,
    boxes, pins, cap, cbin, area,
    feat, hits, send, recv, onehot, early_s, early_r, mid_s, mid_r, fin_s, fin_r, fall, kept,
    in_sem, net_sent, net_got, early_sem, mid_sem, fin_sem,
):
    row = lax.axis_index("row")
    col = lax.axis_index("col")
    tile_r, tile_c = cap.shape
    nets = pins.shape[1]
    cells = cbin.shape[1]
    chunks = nets // LANES
    half = nets // 2

    loads = [
        pltpu.make_async_copy(src, dst, in_sem.at[i])
        for i, (src, dst) in enumerate(
            ((boxes_h, boxes), (pins_h, pins), (cbin_h, cbin), (area_h, area), (cap_h, cap))
        )
    ]
    for load in loads:
        load.start()

    def await_bytes(ref, count, sem):
        some = ref.at[pl.ds(0, count)]
        pltpu.make_async_copy(some, some, sem).wait()

    quad, place4 = col // 4, lax.rem(col, 4)
    member = row * 4 + place4
    plane = [
        (dr, {"row": lax.rem(row + dr, n_row), "col": 4 * quad + lax.rem(place4 + dq, 4)})
        for dr in sorted(range(n_row), key=lambda d: -min(d, n_row - d) - 2 * (d % 2))
        for dq in range(4)
        if dr or dq
    ]

    row_peers = [
        {"row": lax.rem(row + step, n_row)}
        for step in sorted(range(1, n_row), key=lambda d: -min(d, n_row - d) - 2 * (d % 2))
    ]
    plane = [peer for _, peer in plane]

    def push(src, dst, sems, targets):
        for peer in targets:
            pltpu.make_async_remote_copy(
                src_ref=src, dst_ref=dst, send_sem=sems.at[0], recv_sem=sems.at[1],
                device_id=peer, device_id_type=MESH,
            ).start()

    barrier = pltpu.get_barrier_semaphore()
    chips = n_col // 2
    chip, core = col // 2, lax.rem(col, 2)
    far_first = sorted(range(1, chips), key=lambda o: -min(o, chips - o))
    peers = [2 * lax.rem(chip + o, chips) + k for o in far_first for k in range(2)]
    partner = 2 * chip + 1 - core
    peers.append(partner)
    near_first = [0] + far_first[::-1]
    cuts = [0, 5, 9, 13, 16] if chips == 16 else [0, chips]
    groups = [near_first[a:b] for a, b in zip(cuts, cuts[1:])]
    group_of = {o: g for g, group in enumerate(groups) for o in group}
    steps = [o for o in far_first for k in range(2)] + [0]
    for peer in peers:
        pl.semaphore_signal(barrier, inc=1, device_id={"col": peer}, device_id_type=MESH)
    for peer in row_peers:
        pl.semaphore_signal(barrier, inc=1, device_id=peer, device_id_type=MESH)

    loads[0].wait()
    loads[1].wait()
    x0, x1, y0, y1 = (boxes[i : i + 1, :] for i in range(4))
    dx = (x1 - x0 + 1).astype(F32)
    dy = (y1 - y0 + 1).astype(F32)
    weight = jnp.log(pins[...].astype(F32)) * (dx + dy) / (dx * dy)
    weight = weight.astype(BF16).astype(F32)
    row_start = row * tile_r
    y_first = jnp.clip(y0 - row_start, 0, tile_r)
    y_end = jnp.clip(y1 + 1 - row_start, 0, tile_r)
    in_band = jnp.where(y_end > y_first, 1.0, 0.0).astype(F32)
    x_end = x1 + 1
    zero_row = jnp.zeros((1, nets), F32)
    parts = [
        (x0 & -LANES).astype(F32), (x_end & -LANES).astype(F32),
        (y_first & -256).astype(F32), (y_end & -256).astype(F32),
        weight, zero_row, zero_row, zero_row,
        (x0 & (LANES - 1)).astype(F32), (x_end & (LANES - 1)).astype(F32),
        (y_first & 255).astype(F32), (y_end & 255).astype(F32),
        zero_row, zero_row, zero_row, zero_row,
    ]
    for i, part in enumerate(parts):
        feat[i : i + 1, :] = part
    for j in range(chunks):
        hits[j : j + 1, :] = in_band[:, j * LANES : (j + 1) * LANES]
    table = feat[...].astype(BF16)
    marks = hits[...].astype(BF16)
    ci, cj = iota((chunks, chunks), 0), iota((chunks, chunks), 1)
    per_half = chunks // 2
    same_half = jnp.where(ci >= per_half, 1.0, 0.0) == jnp.where(cj >= per_half, 1.0, 0.0)
    ahead = dot(ones_where((ci > cj) & same_half), marks)
    before = ones_where(iota((LANES, LANES), 0) < iota((LANES, LANES), 1))
    place = dot(marks, before) + dot(ahead.astype(BF16), jnp.ones((LANES, LANES), BF16))
    longest = jnp.max(place + hits[...], keepdims=True)
    place = jnp.where((hits[...] > 0.0) & (place < HALF_SLOTS), place, -1.0).astype(BF16)
    slot = iota((HALF_SLOTS, LANES), 0, BF16)
    packed = []
    for h in range(2):
        pick = jnp.concatenate(
            [
                ones_where(slot == jnp.broadcast_to(place[j : j + 1, :], slot.shape))
                for j in range(h * per_half, (h + 1) * per_half)
            ],
            axis=1,
        )
        packed.append(dot_nt(pick, table[:, h * half : (h + 1) * half]).T)
    packed = jnp.concatenate(packed, axis=1)
    listed = packed[0:8] + packed[8:16]
    band_slots = 2 * HALF_SLOTS

    tile_x = iota((n_col, band_slots), 0) * tile_c
    meets = (listed[0:1] < tile_x + tile_c) & (listed[1:2] > tile_x)
    wide = band_slots + LANES
    ti, tj = iota((band_slots, wide), 0), iota((band_slots, wide), 1)
    counted = dot(ones_where(meets), ones_where((ti < tj) | (tj >= band_slots)))
    order = counted[:, :band_slots]
    count = jnp.where(longest > HALF_SLOTS, 1e6, counted[:, band_slots:])
    odd = core.astype(F32)
    order = jnp.where(meets, odd * (SLOTS - 1) + (1.0 - 2.0 * odd) * order, -1.0).astype(BF16)
    slot = iota((SLOTS, band_slots), 0, BF16)
    pick = jnp.concatenate(
        [
            ones_where(slot == jnp.broadcast_to(order[d : d + 1, :], slot.shape))
            for d in range(n_col)
        ],
        axis=0,
    )
    taken = dot_nt(pick, packed.astype(BF16))
    pad = jnp.zeros((LANES - SLOTS, 16), F32)
    line = lax.broadcasted_iota(jnp.int32, (8, LANES), 0)
    lane8 = lax.broadcasted_iota(jnp.int32, (8, LANES), 1)
    count_here = (line == 4) & (lane8 >= SLOTS)
    for d in range(n_col):
        block = jnp.concatenate([taken[d * SLOTS : (d + 1) * SLOTS], pad], axis=0).T
        send[d] = jnp.where(count_here, count[d : d + 1, :], block[0:8] + block[8:16])[0:ROWS]

    pl.semaphore_wait(barrier, n_col - 1 + n_row - 1)
    for peer, o in zip(peers, steps):
        pltpu.make_async_remote_copy(
            src_ref=send.at[peer], dst_ref=recv.at[col],
            send_sem=net_sent, recv_sem=net_got.at[group_of[o]],
            device_id={"col": peer}, device_id_type=MESH,
        ).start()
    recv[col] = send[col]

    loads[2].wait()
    loads[3].wait()
    bins = cbin[...]
    bin_row = (bins // tile_c).astype(F32)
    bin_col = (bins % tile_c).astype(F32)
    for h in range(tile_r // 256):
        onehot[h * 256 : (h + 1) * 256, :] = ones_where(
            iota((256, cells), 0, BF16)
            == jnp.broadcast_to((bin_row - 256.0 * h).astype(BF16), (256, cells))
        )
    in_col = iota((tile_c, cells), 0, BF16) == jnp.broadcast_to(bin_col.astype(BF16), (tile_c, cells))
    area_hi, area_lo = split2(area[...])
    nought = jnp.zeros((), BF16)
    by_col = jnp.concatenate(
        [
            jnp.where(in_col, jnp.broadcast_to(area_hi, (tile_c, cells)), nought),
            jnp.where(in_col, jnp.broadcast_to(area_lo, (tile_c, cells)), nought),
        ],
        axis=0,
    )
    bin_area = dot_nt(onehot[...], by_col)
    bin_area = bin_area[:, :tile_c] + bin_area[:, tile_c:]
    early_s[...] = jnp.sum(bin_area, axis=0, keepdims=True)
    push(early_s, early_r.at[row], early_sem, row_peers)
    early_r[row] = early_s[...]
    w_hi, w_lo = split2(bin_area)
    upper = ones_where(iota((tile_r, tile_r), 0) <= iota((tile_r, tile_r), 1))
    below = dot(upper, jnp.concatenate([w_hi, w_lo], axis=1))
    fall[...] = below[:, :tile_c] + below[:, tile_c:]

    loads[4].wait()
    over = jnp.zeros((1, LANES), F32)
    shift = (col * tile_c).astype(F32)
    lane = lax.broadcasted_iota(jnp.int32, (ROWS, LANES), 1)
    for g, group in enumerate(groups):
        merged = []
        if g == len(groups) - 1:
            await_bytes(early_r, n_row - 1, early_sem.at[1])
            areas_below = jnp.zeros((1, tile_c), F32)
            for r in range(n_row):
                areas_below = areas_below + jnp.where(r > row, early_r[r], 0.0)
            kept[...] = areas_below
        await_bytes(recv, 2 * len(group) - (1 if g == 0 else 0), net_got.at[g])
        for o in group:
            first = 2 * lax.rem(chip + o, chips)
            even, odds = recv[first], recv[first + 1]
            n_even, n_odd = even[4:5], odds[4:5]
            spilt = (n_even > SLOTS) | (n_odd > SLOTS) | (n_even + n_odd > LANES)
            over = over + jnp.where(spilt & (lane[0:1] >= SLOTS), 1.0, 0.0)
            even = jnp.where(lane < SLOTS, even, 0.0)
            odds = jnp.where(lane < SLOTS, odds, 0.0)
            merged.append(even + pltpu.roll(odds, LANES - SLOTS, 1))
        merged = jnp.concatenate(merged, axis=1)
        total = merged.shape[1]
        full = lambda x, n: jnp.broadcast_to(x, (n, total))
        x_lo = jnp.clip(merged[0:1] - shift, 0.0, 1.0 * tile_c).astype(BF16)
        x_hi = jnp.clip(merged[1:2] - shift, 0.0, 1.0 * tile_c).astype(BF16)
        at = iota((tile_c, total), 0, BF16)
        col_weight = jnp.where(
            (at >= full(x_lo, tile_c)) & (at < full(x_hi, tile_c)),
            full(merged[4:5].astype(BF16), tile_c), nought,
        )
        at = iota((256, total), 0, BF16)
        for h in range(tile_r // 256):
            y_lo = jnp.clip(merged[2:3] - 256.0 * h, 0.0, 256.0).astype(BF16)
            y_hi = jnp.clip(merged[3:4] - 256.0 * h, 0.0, 256.0).astype(BF16)
            row_hit = ones_where((at >= full(y_lo, 256)) & (at < full(y_hi, 256)))
            part = dot_nt(row_hit, col_weight)
            rows = slice(h * 256, (h + 1) * 256)
            rudy[rows, :] = part if g == 0 else rudy[rows, :] + part

    excess = jnp.maximum(rudy[...] - cap[...], 0.0)
    column = jnp.sum(excess, axis=0, keepdims=True)
    mid_s[0:1, :] = column
    mid_s[1:2, :] = (
        jnp.sum(excess * fall[...], axis=0, keepdims=True) + column * kept[...] + 1e30 * over
    )
    mid_s[2:3, :] = early_s[...]
    push(mid_s, mid_r.at[member], mid_sem, plane)
    mid_r[member] = mid_s[...]
    e_hi, e_lo = split2(excess)
    lower = ones_where(iota((tile_r, tile_r), 0) >= iota((tile_r, tile_r), 1))
    within = dot(lower, jnp.concatenate([e_hi, e_lo], axis=1))
    infl[...] = within[:, :tile_c] + within[:, tile_c:]
    await_bytes(mid_r, 4 * n_row - 1, mid_sem.at[1])
    parts = [mid_r[m] for m in range(4 * n_row)]
    while len(parts) > 1:
        parts = [a + b for a, b in zip(parts[::2], parts[1::2])]
    factor = 2.0 / (tile_r * n_row)
    fin_s[0:1, :] = parts[0][2:3] + factor * parts[0][1:2]
    fin_s[1:2, :] = parts[0][2:3]
    quads = n_col // 4
    push(
        fin_s, fin_r.at[quad], fin_sem,
        [
            {"col": 4 * lax.rem(quad + dz, quads) + place4}
            for dz in sorted(range(1, quads), key=lambda d: -min(d, quads - d))
        ],
    )
    fin_r[quad] = fin_s[...]
    carried = jnp.zeros((1, tile_c), F32)
    for r in range(n_row):
        carried = carried + jnp.where(r < row, mid_r[4 * r + place4][0:1], 0.0)

    inflation = 1.0 + factor * (infl[...] + carried)
    infl[...] = inflation
    i_hi, i_lo = split2(inflation.T)
    looked = dot(jnp.concatenate([i_hi, i_lo], axis=0), onehot[...])
    looked = looked[:tile_c] + looked[tile_c:]
    in_col = iota((tile_c, cells), 0) == jnp.broadcast_to(bin_col, (tile_c, cells))
    looked = jnp.sum(jnp.where(in_col, looked, 0.0), axis=0, keepdims=True)
    grown[...] = area[...] * looked

    await_bytes(send, n_col - 1, net_sent)
    await_bytes(early_r, n_row - 1, early_sem.at[0])
    await_bytes(mid_r, 4 * n_row - 1, mid_sem.at[0])
    await_bytes(fin_r, quads - 1, fin_sem.at[1])
    parts = [fin_r[c] for c in range(quads)]
    while len(parts) > 1:
        parts = [a + b for a, b in zip(parts[::2], parts[1::2])]
    totals[...] = parts[0]
    await_bytes(fin_r, quads - 1, fin_sem.at[0])


def finish_kernel(rudy, infl, grown, totals, rudy_h, infl_h, sizes_h, flag_h, sizes, flag, sem):
    rows = rudy.shape[0] // PIECES
    stores = []
    for src, dst, done in ((rudy, rudy_h, sem.at[0]), (infl, infl_h, sem.at[1])):
        for i in range(PIECES):
            piece = pl.ds(i * rows, rows)
            pltpu.make_async_copy(src.at[piece], dst.at[piece], done).start()
        stores.append(pltpu.make_async_copy(src, dst, done))
    stores.append(pltpu.make_async_copy(sizes, sizes_h, sem.at[2]))
    stores.append(pltpu.make_async_copy(flag, flag_h, sem.at[3]))
    sums = jnp.sum(totals[...], axis=1, keepdims=True)
    flag[...] = jnp.broadcast_to(sums[0:1], flag.shape)
    stores[3].start()
    sizes[...] = grown[...] * (sums[1:2] / sums[0:1])
    stores[2].start()
    for store in stores:
        store.wait()


def sparse_program(n_row, n_col, boxes, pins, capacity, cell_bin, cell_area):
    tile_r, tile_c = capacity.shape
    nets = pins.shape[0]
    cells = cell_bin.shape[1]
    vm = pltpu.VMEM
    dma = pltpu.SemaphoreType.DMA
    anywhere = pl.BlockSpec(memory_space=pl.ANY)
    inside = pl.BlockSpec(memory_space=pltpu.VMEM)
    shape = jax.ShapeDtypeStruct
    held = pl.pallas_call(
        functools.partial(sparse_kernel, n_row, n_col),
        name="nets_to_tiles",
        out_shape=(
            vm((tile_r, tile_c), F32), vm((tile_r, tile_c), F32),
            vm((1, cells), F32), vm((2, LANES), F32),
        ),
        in_specs=[anywhere] * 5,
        out_specs=(inside,) * 4,
        scratch_shapes=[
            vm((4, nets), jnp.int32), vm((1, nets), jnp.int32), vm((tile_r, tile_c), F32),
            vm((1, cells), jnp.int32), vm((1, cells), F32),
            vm((16, nets), F32), vm((nets // LANES, LANES), F32),
            vm((n_col, ROWS, LANES), F32), vm((n_col, ROWS, LANES), F32),
            vm((tile_r, cells), BF16),
            vm((1, tile_c), F32), vm((n_row, 1, tile_c), F32),
            vm((3, tile_c), F32), vm((4 * n_row, 3, tile_c), F32),
            vm((2, tile_c), F32), vm((n_col // 4, 2, tile_c), F32),
            vm((tile_r, tile_c), F32), vm((1, tile_c), F32),
            dma((5,)), dma(()), dma((4,)), dma((2,)), dma((2,)), dma((2,)),
        ],
        compiler_params=pltpu.CompilerParams(
            collective_id=0, has_side_effects=True, vmem_limit_bytes=24 * 1024 * 1024
        ),
    )(boxes, pins.reshape(1, nets), capacity, cell_bin, cell_area)
    return pl.pallas_call(
        finish_kernel,
        name="finish",
        out_shape=(
            shape((tile_r, tile_c), F32), shape((tile_r, tile_c), F32), shape((1, cells), F32),
            shape((1, LANES), F32),
        ),
        in_specs=[inside] * 4,
        out_specs=(anywhere,) * 4,
        scratch_shapes=[vm((1, cells), F32), vm((1, LANES), F32), dma((4,))],
        compiler_params=pltpu.CompilerParams(vmem_limit_bytes=4 * 1024 * 1024),
    )(*held)


def to_everyone(shard, axis):
    peers = lax.axis_size(axis)
    return lax.all_to_all(
        jnp.broadcast_to(shard[None], (peers, *shard.shape)), axis, 0, 0, tiled=True
    )


def dense_program(boxes, pins, capacity, cell_bin, cell_area):
    tile_rows, tile_cols = capacity.shape
    table = jnp.concatenate([boxes, pins[None, :]], axis=0)
    table = to_everyone(table, "col")
    rows_here = lax.axis_index("row") * tile_rows + jnp.arange(tile_rows, dtype=jnp.int32)
    cols_here = lax.axis_index("col") * tile_cols + jnp.arange(tile_cols, dtype=jnp.int32)

    def add_block(index, acc):
        first_x, last_x, first_y, last_y, pin = table[index]
        span_x = (last_x - first_x + 1).astype(F32)
        span_y = (last_y - first_y + 1).astype(F32)
        weight = jnp.log(pin.astype(F32)) * (span_x + span_y) / (span_x * span_y)
        row_hits = (rows_here[:, None] >= first_y[None, :]) & (rows_here[:, None] <= last_y[None, :])
        col_hits = (cols_here[:, None] >= first_x[None, :]) & (cols_here[:, None] <= last_x[None, :])
        weighted = jnp.where(col_hits, weight.astype(BF16)[None, :], jnp.zeros((), BF16))
        return acc + dot_nt(row_hits.astype(BF16), weighted)

    rudy = lax.fori_loop(
        0, table.shape[0], add_block, jnp.zeros((tile_rows, tile_cols), F32)
    )
    excess = jnp.maximum(rudy - capacity, 0.0)
    ladder = jnp.arange(tile_rows, dtype=jnp.int32)
    lower = (ladder[:, None] >= ladder[None, :]).astype(F32)
    within = jnp.dot(
        lower, excess, precision=lax.Precision.HIGHEST, preferred_element_type=F32
    )
    sums = to_everyone(within[-1][None, :], "row")[:, 0]
    above = jnp.arange(sums.shape[0], dtype=jnp.int32) < lax.axis_index("row")
    carried = jnp.sum(jnp.where(above[:, None], sums, 0.0), axis=0)
    inflation = 1.0 + 2.0 * (within + carried[None, :]) / (tile_rows * lax.axis_size("row"))
    looked = jnp.take(inflation.reshape(-1), cell_bin[0], axis=0)
    grown = cell_area * looked[None, :]
    totals = jnp.stack([jnp.sum(cell_area), jnp.sum(grown)])[None, :]
    for axis in ("row", "col"):
        totals = jnp.sum(to_everyone(totals, axis), axis=0)
    cell_sizes = grown * (totals[0, 0] / totals[0, 1])
    return rudy, inflation, cell_sizes


def per_device(n_row, n_col, *args):
    rudy, inflation, cell_sizes, flag = sparse_program(n_row, n_col, *args)

    def again(state):
        held = [jnp.where(state[3][0, 0] > 1e20, x, jnp.ones((), x.dtype)) for x in args]
        return (*dense_program(*held), jnp.zeros_like(flag))

    state = lax.while_loop(
        lambda state: state[3][0, 0] > 1e20, again, (rudy, inflation, cell_sizes, flag)
    )
    return state[:3]


def solution(mesh):
    n_row, n_col = mesh.shape["row"], mesh.shape["col"]
    placed = (P(None, "col"), P("col"), P("row", "col"), P("row", "col"), P("row", "col"))
    return jax.shard_map(
        functools.partial(per_device, n_row, n_col),
        mesh=mesh,
        in_specs=placed,
        out_specs=(P("row", "col"),) * 3,
        check_vma=False,
    )
```

```python
import functools

import jax
import jax.numpy as jnp
from jax import lax
from jax.experimental import pallas as pl
from jax.experimental.pallas import tpu as pltpu
from jax.sharding import PartitionSpec as P

MESH = pl.DeviceIdType.MESH
F32 = jnp.float32
BF16 = jnp.bfloat16
SLOTS = 80
ROWS = 5
PIECES = 4
HALF_SLOTS = 256
LANES = 128


def iota(shape, dim, dtype=F32):
    return lax.broadcasted_iota(jnp.int32, shape, dim).astype(dtype)


def ones_where(mask, dtype=BF16):
    return jnp.where(mask, jnp.ones((), dtype), jnp.zeros((), dtype))


def dot(a, b):
    return lax.dot_general(a, b, (((1,), (0,)), ((), ())), preferred_element_type=F32)


def dot_nt(a, b):
    return lax.dot_general(a, b, (((1,), (1,)), ((), ())), preferred_element_type=F32)


def split2(x):
    hi = x.astype(BF16)
    return hi, (x - hi.astype(F32)).astype(BF16)


def sparse_kernel(
    n_row, n_col,
    boxes_h, pins_h, cap_h, cbin_h, area_h,
    rudy, infl, grown, totals,
    boxes, pins, cap, cbin, area,
    feat, hits, ahead_or_all, lists, swapped, send, recv, spill, onehot, early_s, early_r, mid_s, mid_r, fin_s, fin_r, fall, kept,
    in_sem, swap_sem, net_sent, net_got, early_sem, mid_sem, fin_sem,
):
    row = lax.axis_index("row")
    col = lax.axis_index("col")
    tile_r, tile_c = cap.shape
    nets = pins.shape[1]
    cells = cbin.shape[1]
    chunks = nets // LANES
    half = nets // 2

    loads = [
        pltpu.make_async_copy(src, dst, in_sem.at[i])
        for i, (src, dst) in enumerate(
            ((boxes_h, boxes), (pins_h, pins), (cbin_h, cbin), (area_h, area), (cap_h, cap))
        )
    ]
    for load in loads:
        load.start()

    def await_bytes(ref, count, sem):
        some = ref.at[pl.ds(0, count)]
        pltpu.make_async_copy(some, some, sem).wait()

    quad, place4 = col // 4, lax.rem(col, 4)
    member = row * 4 + place4
    plane = [
        {"row": lax.rem(row + dr, n_row), "col": 4 * quad + lax.rem(place4 + dq, 4)}
        for dr, dq in sorted(
            [(dr, dq) for dr in range(n_row) for dq in range(4) if dr or dq],
            key=lambda d: -min(d[0], n_row - d[0]) / 2 - 2 * (d[0] % 2) - 1.5 * (d[1] % 2),
        )
    ]

    row_peers = [
        {"row": lax.rem(row + step, n_row)}
        for step in sorted(range(1, n_row), key=lambda d: -min(d, n_row - d) - 2 * (d % 2))
    ]

    def push(src, dst, sems, targets):
        for peer in targets:
            pltpu.make_async_remote_copy(
                src_ref=src, dst_ref=dst, send_sem=sems.at[0], recv_sem=sems.at[1],
                device_id=peer, device_id_type=MESH,
            ).start()

    barrier = pltpu.get_barrier_semaphore()
    chips = n_col // 2
    chip, core = col // 2, lax.rem(col, 2)
    far_first = sorted(range(1, chips), key=lambda o: -min(o, chips - o))
    chip_peers = [(o, lax.rem(chip + o, chips)) for o in far_first]
    partner = {"col": 2 * chip + 1 - core}
    for _, peer in chip_peers:
        pl.semaphore_signal(
            barrier, inc=1, device_id={"col": 2 * peer + core}, device_id_type=MESH
        )
    pl.semaphore_signal(barrier, inc=1, device_id=partner, device_id_type=MESH)
    near_first = [0] + far_first[::-1]
    cuts = [0, 5, 9, 13, 16] if chips == 16 else [0, chips]
    groups = [near_first[a:b] for a, b in zip(cuts, cuts[1:])]
    group_of = {o: g for g, group in enumerate(groups) for o in group}
    for peer in row_peers:
        pl.semaphore_signal(barrier, inc=1, device_id=peer, device_id_type=MESH)

    band_slots = 2 * HALF_SLOTS
    wide = band_slots + LANES
    ti, tj = iota((band_slots, wide), 0), iota((band_slots, wide), 1)
    ahead_or_all[...] = jnp.where(tj >= band_slots, 1.0, jnp.where(ti < tj, 1.0, 0.0)).astype(BF16)

    loads[0].wait()
    loads[1].wait()
    x0, x1, y0, y1 = (boxes[i : i + 1, :] for i in range(4))
    dx = (x1 - x0 + 1).astype(F32)
    dy = (y1 - y0 + 1).astype(F32)
    weight = jnp.log(pins[...].astype(F32)) * (dx + dy) / (dx * dy)
    weight = weight.astype(BF16).astype(F32)
    row_start = row * tile_r
    y_first = jnp.clip(y0 - row_start, 0, tile_r)
    y_end = jnp.clip(y1 + 1 - row_start, 0, tile_r)
    in_band = jnp.where(y_end > y_first, 1.0, 0.0).astype(F32)
    x_end = x1 + 1
    zero_row = jnp.zeros((1, nets), F32)
    parts = [
        (x0 & -LANES).astype(F32), (x_end & -LANES).astype(F32),
        (y_first & -256).astype(F32), (y_end & -256).astype(F32),
        weight, zero_row, zero_row, zero_row,
        (x0 & (LANES - 1)).astype(F32), (x_end & (LANES - 1)).astype(F32),
        (y_first & 255).astype(F32), (y_end & 255).astype(F32),
        zero_row, zero_row, zero_row, zero_row,
    ]
    for i, part in enumerate(parts):
        feat[i : i + 1, :] = part
    for j in range(chunks):
        hits[j : j + 1, :] = in_band[:, j * LANES : (j + 1) * LANES]
    table = feat[...].astype(BF16)
    marks = hits[...].astype(BF16)
    ci, cj = iota((chunks, chunks), 0), iota((chunks, chunks), 1)
    per_half = chunks // 2
    same_half = jnp.where(ci >= per_half, 1.0, 0.0) == jnp.where(cj >= per_half, 1.0, 0.0)
    ahead = dot(ones_where((ci > cj) & same_half), marks)
    before = ones_where(iota((LANES, LANES), 0) < iota((LANES, LANES), 1))
    place = dot(marks, before) + dot(ahead.astype(BF16), jnp.ones((LANES, LANES), BF16))
    longest = jnp.max(place + hits[...], keepdims=True)
    place = jnp.where((hits[...] > 0.0) & (place < HALF_SLOTS), place, -1.0).astype(BF16)
    slot = iota((HALF_SLOTS, LANES), 0, BF16)
    packed = []
    for h in range(2):
        pick = jnp.concatenate(
            [
                ones_where(slot == jnp.broadcast_to(place[j : j + 1, :], slot.shape))
                for j in range(h * per_half, (h + 1) * per_half)
            ],
            axis=1,
        )
        packed.append(dot_nt(pick, table[:, h * half : (h + 1) * half]).T)
    packed = jnp.concatenate(packed, axis=1)
    listed = packed[0:8] + packed[8:16]

    tile_x = iota((n_col, band_slots), 0) * tile_c
    meets = (listed[0:1] < tile_x + tile_c) & (listed[1:2] > tile_x)
    counted = dot(ones_where(meets), ahead_or_all[...])
    order = counted[:, :band_slots]
    count = jnp.where(longest > HALF_SLOTS, 1e6, counted[:, band_slots:])
    odd = core.astype(F32)
    order = jnp.where(meets, odd * (SLOTS - 1) + (1.0 - 2.0 * odd) * order, -1.0).astype(BF16)
    slot = iota((SLOTS, band_slots), 0, BF16)
    share = min(8, chips)
    packed = jnp.concatenate([packed.astype(BF16)] * share, axis=0)
    pad = jnp.zeros((LANES - SLOTS, 16 * share), F32)
    lane16 = lax.broadcasted_iota(jnp.int32, (SLOTS, 16 * share), 1)
    line = lax.broadcasted_iota(jnp.int32, (8, LANES), 0)
    taken = []
    for parity in range(2):
        pick = jnp.concatenate(
            [
                ones_where(slot == jnp.broadcast_to(order[d : d + 1, :], slot.shape))
                for d in range(parity, n_col, 2)
            ],
            axis=0,
        )
        taken.append(dot_nt(pick, packed))
    for first in range(0, chips, share):
        for parity in range(2):
            mixed = taken[parity][first * SLOTS : (first + 1) * SLOTS]
            for j in range(1, share):
                rows = slice((first + j) * SLOTS, (first + j + 1) * SLOTS)
                mixed = jnp.where(lane16 >= 16 * j, taken[parity][rows], mixed)
            turned = jnp.concatenate([mixed, pad], axis=0).T
            for j in range(share):
                d = 2 * (first + j) + parity
                block = turned[16 * j : 16 * j + 8] + turned[16 * j + 8 : 16 * j + 16]
                block = pltpu.roll(block, core * (LANES - SLOTS), 1)
                block = jnp.where(line == ROWS, count[d : d + 1, :], block)
                lists[parity, first + j] = block[0 : ROWS + 1]

    loads[2].wait()
    loads[3].wait()
    bins = cbin[...]
    bin_row = (bins // tile_c).astype(F32)
    bin_col = (bins % tile_c).astype(F32)
    for h in range(tile_r // 256):
        onehot[h * 256 : (h + 1) * 256, :] = ones_where(
            iota((256, cells), 0, BF16)
            == jnp.broadcast_to((bin_row - 256.0 * h).astype(BF16), (256, cells))
        )
    in_col = iota((tile_c, cells), 0, BF16) == jnp.broadcast_to(bin_col.astype(BF16), (tile_c, cells))
    area_hi, area_lo = split2(area[...])
    nought = jnp.zeros((), BF16)
    by_col = jnp.concatenate(
        [
            jnp.where(in_col, jnp.broadcast_to(area_hi, (tile_c, cells)), nought),
            jnp.where(in_col, jnp.broadcast_to(area_lo, (tile_c, cells)), nought),
        ],
        axis=0,
    )
    bin_area = dot_nt(onehot[...], by_col)
    bin_area = bin_area[:, :tile_c] + bin_area[:, tile_c:]
    early_s[...] = jnp.sum(bin_area, axis=0, keepdims=True)

    pl.semaphore_wait(barrier, chips + n_row - 1)
    swap = pltpu.make_async_remote_copy(
        src_ref=lists.at[1 - core], dst_ref=swapped, send_sem=swap_sem.at[0],
        recv_sem=swap_sem.at[1], device_id=partner, device_id_type=MESH,
    )
    swap.start()
    push(early_s, early_r.at[row], early_sem, row_peers)
    early_r[row] = early_s[...]
    swap.wait_recv()
    for p in range(chips):
        send[p] = (lists[core, p] + swapped[p])[0:ROWS]
    for o, peer in chip_peers:
        pltpu.make_async_remote_copy(
            src_ref=send.at[peer], dst_ref=recv.at[chip],
            send_sem=net_sent, recv_sem=net_got.at[group_of[o]],
            device_id={"col": 2 * peer + core}, device_id_type=MESH,
        ).start()
    recv[chip] = send[chip]
    over = jnp.zeros((1, LANES), F32)
    for p in range(chips):
        ours, theirs = lists[core, p][ROWS:], swapped[p][ROWS:]
        spilt = (ours > SLOTS) | (theirs > SLOTS) | (ours + theirs > LANES)
        over = over + jnp.where(spilt, 1.0, 0.0)
    spill[...] = over

    await_bytes(early_r, n_row - 1, early_sem.at[0])
    w_hi, w_lo = split2(bin_area)
    upper = ones_where(iota((tile_r, tile_r), 0) <= iota((tile_r, tile_r), 1))
    below = dot(upper, jnp.concatenate([w_hi, w_lo], axis=1))
    fall[...] = below[:, :tile_c] + below[:, tile_c:]

    loads[4].wait()
    shift = (col * tile_c).astype(F32)
    for g, group in enumerate(groups):
        if g == len(groups) - 1:
            await_bytes(early_r, n_row - 1, early_sem.at[1])
            areas_below = jnp.zeros((1, tile_c), F32)
            for r in range(n_row):
                areas_below = areas_below + jnp.where(r > row, early_r[r], 0.0)
            kept[...] = areas_below
        await_bytes(recv, len(group) - (1 if g == 0 else 0), net_got.at[g])
        merged = [recv[lax.rem(chip + o, chips)] for o in group]
        merged = jnp.concatenate(merged, axis=1)
        total = merged.shape[1]
        full = lambda x, n: jnp.broadcast_to(x, (n, total))
        x_lo = jnp.clip(merged[0:1] - shift, 0.0, 1.0 * tile_c).astype(BF16)
        x_hi = jnp.clip(merged[1:2] - shift, 0.0, 1.0 * tile_c).astype(BF16)
        at = iota((tile_c, total), 0, BF16)
        col_weight = jnp.where(
            (at >= full(x_lo, tile_c)) & (at < full(x_hi, tile_c)),
            full(merged[4:5].astype(BF16), tile_c), nought,
        )
        at = iota((256, total), 0, BF16)
        for h in range(tile_r // 256):
            y_lo = jnp.clip(merged[2:3] - 256.0 * h, 0.0, 256.0).astype(BF16)
            y_hi = jnp.clip(merged[3:4] - 256.0 * h, 0.0, 256.0).astype(BF16)
            row_hit = ones_where((at >= full(y_lo, 256)) & (at < full(y_hi, 256)))
            part = dot_nt(row_hit, col_weight)
            rows = slice(h * 256, (h + 1) * 256)
            rudy[rows, :] = part if g == 0 else rudy[rows, :] + part

    excess = jnp.maximum(rudy[...] - cap[...], 0.0)
    column = jnp.sum(excess, axis=0, keepdims=True)
    mid_s[0:1, :] = column
    mid_s[1:2, :] = (
        jnp.sum(excess * fall[...], axis=0, keepdims=True) + column * kept[...]
        + 1e30 * spill[...]
    )
    mid_s[2:3, :] = early_s[...]
    push(mid_s, mid_r.at[member], mid_sem, plane)
    mid_r[member] = mid_s[...]
    swap.wait_send()
    e_hi, e_lo = split2(jnp.maximum(rudy[...] - cap[...], 0.0))
    lower = ones_where(iota((tile_r, tile_r), 0) >= iota((tile_r, tile_r), 1))
    within = dot(lower, jnp.concatenate([e_hi, e_lo], axis=1))
    infl[...] = within[:, :tile_c] + within[:, tile_c:]
    await_bytes(mid_r, 4 * n_row - 1, mid_sem.at[1])
    parts = [mid_r[m] for m in range(4 * n_row)]
    while len(parts) > 1:
        parts = [a + b for a, b in zip(parts[::2], parts[1::2])]
    factor = 2.0 / (tile_r * n_row)
    fin_s[0:1, :] = parts[0][2:3] + factor * parts[0][1:2]
    fin_s[1:2, :] = parts[0][2:3]
    quads = n_col // 4
    push(
        fin_s, fin_r.at[quad], fin_sem,
        [
            {"col": 4 * lax.rem(quad + dz, quads) + place4}
            for dz in sorted(range(1, quads), key=lambda d: -min(d, quads - d))
        ],
    )
    fin_r[quad] = fin_s[...]
    carried = jnp.zeros((1, tile_c), F32)
    for r in range(n_row):
        carried = carried + jnp.where(r < row, mid_r[4 * r + place4][0:1], 0.0)

    inflation = 1.0 + factor * (infl[...] + carried)
    infl[...] = inflation
    i_hi, i_lo = split2(inflation.T)
    looked = dot(jnp.concatenate([i_hi, i_lo], axis=0), onehot[...])
    looked = looked[:tile_c] + looked[tile_c:]
    in_col = iota((tile_c, cells), 0) == jnp.broadcast_to(bin_col, (tile_c, cells))
    looked = jnp.sum(jnp.where(in_col, looked, 0.0), axis=0, keepdims=True)
    grown[...] = area[...] * looked

    await_bytes(send, chips - 1, net_sent)
    await_bytes(mid_r, 4 * n_row - 1, mid_sem.at[0])
    await_bytes(fin_r, quads - 1, fin_sem.at[1])
    parts = [fin_r[c] for c in range(quads)]
    while len(parts) > 1:
        parts = [a + b for a, b in zip(parts[::2], parts[1::2])]
    totals[...] = parts[0]
    await_bytes(fin_r, quads - 1, fin_sem.at[0])


def finish_kernel(rudy, infl, grown, totals, rudy_h, infl_h, sizes_h, flag_h, sizes, flag, sem):
    rows = rudy.shape[0] // PIECES
    stores = []
    for src, dst, done in ((rudy, rudy_h, sem.at[0]), (infl, infl_h, sem.at[1])):
        for i in range(PIECES):
            piece = pl.ds(i * rows, rows)
            pltpu.make_async_copy(src.at[piece], dst.at[piece], done).start()
        stores.append(pltpu.make_async_copy(src, dst, done))
    stores.append(pltpu.make_async_copy(sizes, sizes_h, sem.at[2]))
    stores.append(pltpu.make_async_copy(flag, flag_h, sem.at[3]))
    sums = jnp.sum(totals[...], axis=1, keepdims=True)
    flag[...] = jnp.broadcast_to(sums[0:1], flag.shape)
    stores[3].start()
    sizes[...] = grown[...] * (sums[1:2] / sums[0:1])
    stores[2].start()
    for store in stores:
        store.wait()


def sparse_program(n_row, n_col, boxes, pins, capacity, cell_bin, cell_area):
    tile_r, tile_c = capacity.shape
    nets = pins.shape[0]
    cells = cell_bin.shape[1]
    vm = pltpu.VMEM
    dma = pltpu.SemaphoreType.DMA
    anywhere = pl.BlockSpec(memory_space=pl.ANY)
    inside = pl.BlockSpec(memory_space=pltpu.VMEM)
    shape = jax.ShapeDtypeStruct
    held = pl.pallas_call(
        functools.partial(sparse_kernel, n_row, n_col),
        name="nets_to_tiles",
        out_shape=(
            vm((tile_r, tile_c), F32), vm((tile_r, tile_c), F32),
            vm((1, cells), F32), vm((2, LANES), F32),
        ),
        in_specs=[anywhere] * 5,
        out_specs=(inside,) * 4,
        scratch_shapes=[
            vm((4, nets), jnp.int32), vm((1, nets), jnp.int32), vm((tile_r, tile_c), F32),
            vm((1, cells), jnp.int32), vm((1, cells), F32),
            vm((16, nets), F32), vm((nets // LANES, LANES), F32),
            vm((2 * HALF_SLOTS, 2 * HALF_SLOTS + LANES), BF16),
            vm((2, n_col // 2, ROWS + 1, LANES), F32), vm((n_col // 2, ROWS + 1, LANES), F32),
            vm((n_col // 2, ROWS, LANES), F32), vm((n_col // 2, ROWS, LANES), F32),
            vm((1, LANES), F32),
            vm((tile_r, cells), BF16),
            vm((1, tile_c), F32), vm((n_row, 1, tile_c), F32),
            vm((3, tile_c), F32), vm((4 * n_row, 3, tile_c), F32),
            vm((2, tile_c), F32), vm((n_col // 4, 2, tile_c), F32),
            vm((tile_r, tile_c), F32), vm((1, tile_c), F32),
            dma((5,)), dma((2,)), dma(()), dma((4,)), dma((2,)), dma((2,)), dma((2,)),
        ],
        compiler_params=pltpu.CompilerParams(
            collective_id=0, has_side_effects=True, vmem_limit_bytes=24 * 1024 * 1024
        ),
    )(boxes, pins.reshape(1, nets), capacity, cell_bin, cell_area)
    return pl.pallas_call(
        finish_kernel,
        name="finish",
        out_shape=(
            shape((tile_r, tile_c), F32), shape((tile_r, tile_c), F32), shape((1, cells), F32),
            shape((1, LANES), F32),
        ),
        in_specs=[inside] * 4,
        out_specs=(anywhere,) * 4,
        scratch_shapes=[vm((1, cells), F32), vm((1, LANES), F32), dma((4,))],
        compiler_params=pltpu.CompilerParams(vmem_limit_bytes=4 * 1024 * 1024),
    )(*held)


def to_everyone(shard, axis):
    peers = lax.axis_size(axis)
    return lax.all_to_all(
        jnp.broadcast_to(shard[None], (peers, *shard.shape)), axis, 0, 0, tiled=True
    )


def dense_program(boxes, pins, capacity, cell_bin, cell_area):
    tile_rows, tile_cols = capacity.shape
    table = jnp.concatenate([boxes, pins[None, :]], axis=0)
    table = to_everyone(table, "col")
    rows_here = lax.axis_index("row") * tile_rows + jnp.arange(tile_rows, dtype=jnp.int32)
    cols_here = lax.axis_index("col") * tile_cols + jnp.arange(tile_cols, dtype=jnp.int32)

    def add_block(index, acc):
        first_x, last_x, first_y, last_y, pin = table[index]
        span_x = (last_x - first_x + 1).astype(F32)
        span_y = (last_y - first_y + 1).astype(F32)
        weight = jnp.log(pin.astype(F32)) * (span_x + span_y) / (span_x * span_y)
        row_hits = (rows_here[:, None] >= first_y[None, :]) & (rows_here[:, None] <= last_y[None, :])
        col_hits = (cols_here[:, None] >= first_x[None, :]) & (cols_here[:, None] <= last_x[None, :])
        weighted = jnp.where(col_hits, weight.astype(BF16)[None, :], jnp.zeros((), BF16))
        return acc + dot_nt(row_hits.astype(BF16), weighted)

    rudy = lax.fori_loop(
        0, table.shape[0], add_block, jnp.zeros((tile_rows, tile_cols), F32)
    )
    excess = jnp.maximum(rudy - capacity, 0.0)
    ladder = jnp.arange(tile_rows, dtype=jnp.int32)
    lower = (ladder[:, None] >= ladder[None, :]).astype(F32)
    within = jnp.dot(
        lower, excess, precision=lax.Precision.HIGHEST, preferred_element_type=F32
    )
    sums = to_everyone(within[-1][None, :], "row")[:, 0]
    above = jnp.arange(sums.shape[0], dtype=jnp.int32) < lax.axis_index("row")
    carried = jnp.sum(jnp.where(above[:, None], sums, 0.0), axis=0)
    inflation = 1.0 + 2.0 * (within + carried[None, :]) / (tile_rows * lax.axis_size("row"))
    looked = jnp.take(inflation.reshape(-1), cell_bin[0], axis=0)
    grown = cell_area * looked[None, :]
    totals = jnp.stack([jnp.sum(cell_area), jnp.sum(grown)])[None, :]
    for axis in ("row", "col"):
        totals = jnp.sum(to_everyone(totals, axis), axis=0)
    cell_sizes = grown * (totals[0, 0] / totals[0, 1])
    return rudy, inflation, cell_sizes


def per_device(n_row, n_col, *args):
    rudy, inflation, cell_sizes, flag = sparse_program(n_row, n_col, *args)

    def again(state):
        held = [jnp.where(state[3][0, 0] > 1e20, x, jnp.ones((), x.dtype)) for x in args]
        return (*dense_program(*held), jnp.zeros_like(flag))

    state = lax.while_loop(
        lambda state: state[3][0, 0] > 1e20, again, (rudy, inflation, cell_sizes, flag)
    )
    return state[:3]


def solution(mesh):
    n_row, n_col = mesh.shape["row"], mesh.shape["col"]
    placed = (P(None, "col"), P("col"), P("row", "col"), P("row", "col"), P("row", "col"))
    return jax.shard_map(
        functools.partial(per_device, n_row, n_col),
        mesh=mesh,
        in_specs=placed,
        out_specs=(P("row", "col"),) * 3,
        check_vma=False,
    )
```

```python
import functools

import jax
import jax.numpy as jnp
from jax import lax
from jax.experimental import pallas as pl
from jax.experimental.pallas import tpu as pltpu
from jax.sharding import PartitionSpec as P

MESH = pl.DeviceIdType.MESH
F32 = jnp.float32
BF16 = jnp.bfloat16
SLOTS = 80
ROWS = 5
PIECES = 4
HALF_SLOTS = 256
LANES = 128


def iota(shape, dim, dtype=F32):
    return lax.broadcasted_iota(jnp.int32, shape, dim).astype(dtype)


def ones_where(mask, dtype=BF16):
    return jnp.where(mask, jnp.ones((), dtype), jnp.zeros((), dtype))


def dot(a, b):
    return lax.dot_general(a, b, (((1,), (0,)), ((), ())), preferred_element_type=F32)


def dot_nt(a, b):
    return lax.dot_general(a, b, (((1,), (1,)), ((), ())), preferred_element_type=F32)


def split2(x):
    hi = x.astype(BF16)
    return hi, (x - hi.astype(F32)).astype(BF16)


def sparse_kernel(
    n_row, n_col,
    boxes_h, pins_h, cap_h, cbin_h, area_h,
    rudy, infl, grown, totals,
    boxes, pins, cap, cbin, area,
    feat, hits, ahead_or_all, lists, swapped, send, recv, spill, onehot, early_s, early_r, mid_s, mid_r, fin_s, fin_r, fall, kept,
    in_sem, swap_sem, net_sent, net_got, early_sem, mid_sem, fin_sem,
):
    row = lax.axis_index("row")
    col = lax.axis_index("col")
    tile_r, tile_c = cap.shape
    nets = pins.shape[1]
    cells = cbin.shape[1]
    chunks = nets // LANES
    half = nets // 2

    loads = [
        pltpu.make_async_copy(src, dst, in_sem.at[i])
        for i, (src, dst) in enumerate(
            ((boxes_h, boxes), (pins_h, pins), (cbin_h, cbin), (area_h, area), (cap_h, cap))
        )
    ]
    for load in loads:
        load.start()

    def await_bytes(ref, count, sem):
        some = ref.at[pl.ds(0, count)]
        pltpu.make_async_copy(some, some, sem).wait()

    quad, place4 = col // 4, lax.rem(col, 4)
    member = row * 4 + place4
    plane = [
        {"row": lax.rem(row + dr, n_row), "col": 4 * quad + lax.rem(place4 + dq, 4)}
        for dr, dq in sorted(
            [(dr, dq) for dr in range(n_row) for dq in range(4) if dr or dq],
            key=lambda d: -min(d[0], n_row - d[0]) / 2 - 2 * (d[0] % 2) - 1.5 * (d[1] % 2),
        )
    ]

    row_peers = [
        {"row": lax.rem(row + step, n_row)}
        for step in sorted(range(1, n_row), key=lambda d: -min(d, n_row - d) - 2 * (d % 2))
    ]

    def push(src, dst, sems, targets):
        for peer in targets:
            pltpu.make_async_remote_copy(
                src_ref=src, dst_ref=dst, send_sem=sems.at[0], recv_sem=sems.at[1],
                device_id=peer, device_id_type=MESH,
            ).start()

    barrier = pltpu.get_barrier_semaphore()
    chips = n_col // 2
    chip, core = col // 2, lax.rem(col, 2)
    far_first = sorted(range(1, chips), key=lambda o: -min(o, chips - o))
    chip_peers = [(o, lax.rem(chip + o, chips)) for o in far_first]
    partner = {"col": 2 * chip + 1 - core}
    for _, peer in chip_peers:
        pl.semaphore_signal(
            barrier, inc=1, device_id={"col": 2 * peer + core}, device_id_type=MESH
        )
    pl.semaphore_signal(barrier, inc=1, device_id=partner, device_id_type=MESH)
    near_first = [0] + far_first[::-1]
    cuts = [0, 5, 9, 13, 16] if chips == 16 else [0, chips]
    groups = [near_first[a:b] for a, b in zip(cuts, cuts[1:])]
    group_of = {o: g for g, group in enumerate(groups) for o in group}
    for peer in row_peers:
        pl.semaphore_signal(barrier, inc=1, device_id=peer, device_id_type=MESH)

    band_slots = 2 * HALF_SLOTS
    wide = band_slots + LANES
    ti, tj = iota((band_slots, wide), 0), iota((band_slots, wide), 1)
    ahead_or_all[...] = jnp.where(tj >= band_slots, 1.0, jnp.where(ti < tj, 1.0, 0.0)).astype(BF16)

    loads[0].wait()
    loads[1].wait()
    x0, x1, y0, y1 = (boxes[i : i + 1, :] for i in range(4))
    dx = (x1 - x0 + 1).astype(F32)
    dy = (y1 - y0 + 1).astype(F32)
    weight = jnp.log(pins[...].astype(F32)) * (dx + dy) / (dx * dy)
    weight = weight.astype(BF16).astype(F32)
    row_start = row * tile_r
    y_first = jnp.clip(y0 - row_start, 0, tile_r)
    y_end = jnp.clip(y1 + 1 - row_start, 0, tile_r)
    in_band = jnp.where(y_end > y_first, 1.0, 0.0).astype(F32)
    x_end = x1 + 1
    zero_row = jnp.zeros((1, nets), F32)
    parts = [
        (x0 & -LANES).astype(F32), (x_end & -LANES).astype(F32),
        (y_first & -256).astype(F32), (y_end & -256).astype(F32),
        weight, zero_row, zero_row, zero_row,
        (x0 & (LANES - 1)).astype(F32), (x_end & (LANES - 1)).astype(F32),
        (y_first & 255).astype(F32), (y_end & 255).astype(F32),
        zero_row, zero_row, zero_row, zero_row,
    ]
    for i, part in enumerate(parts):
        feat[i : i + 1, :] = part
    for j in range(chunks):
        hits[j : j + 1, :] = in_band[:, j * LANES : (j + 1) * LANES]
    table = feat[...].astype(BF16)
    marks = hits[...].astype(BF16)
    ci, cj = iota((chunks, chunks), 0), iota((chunks, chunks), 1)
    per_half = chunks // 2
    same_half = jnp.where(ci >= per_half, 1.0, 0.0) == jnp.where(cj >= per_half, 1.0, 0.0)
    ahead = dot(ones_where((ci > cj) & same_half), marks)
    before = ones_where(iota((LANES, LANES), 0) < iota((LANES, LANES), 1))
    place = dot(marks, before) + dot(ahead.astype(BF16), jnp.ones((LANES, LANES), BF16))
    longest = jnp.max(place + hits[...], keepdims=True)
    place = jnp.where((hits[...] > 0.0) & (place < HALF_SLOTS), place, -1.0).astype(BF16)
    slot = iota((HALF_SLOTS, LANES), 0, BF16)
    packed = []
    for h in range(2):
        pick = jnp.concatenate(
            [
                ones_where(slot == jnp.broadcast_to(place[j : j + 1, :], slot.shape))
                for j in range(h * per_half, (h + 1) * per_half)
            ],
            axis=1,
        )
        packed.append(dot_nt(pick, table[:, h * half : (h + 1) * half]).T)
    packed = jnp.concatenate(packed, axis=1)
    listed = packed[0:8] + packed[8:16]

    tile_x = iota((n_col, band_slots), 0) * tile_c
    meets = (listed[0:1] < tile_x + tile_c) & (listed[1:2] > tile_x)
    counted = dot(ones_where(meets), ahead_or_all[...])
    order = counted[:, :band_slots]
    count = jnp.where(longest > HALF_SLOTS, 1e6, counted[:, band_slots:])
    odd = core.astype(F32)
    order = jnp.where(meets, odd * (SLOTS - 1) + (1.0 - 2.0 * odd) * order, -1.0).astype(BF16)
    slot = iota((SLOTS, band_slots), 0, BF16)
    share = min(8, chips)
    packed = jnp.concatenate([packed.astype(BF16)] * share, axis=0)
    pad = jnp.zeros((LANES - SLOTS, 16 * share), F32)
    lane16 = lax.broadcasted_iota(jnp.int32, (SLOTS, 16 * share), 1)
    line = lax.broadcasted_iota(jnp.int32, (8, LANES), 0)
    taken = []
    for parity in range(2):
        pick = jnp.concatenate(
            [
                ones_where(slot == jnp.broadcast_to(order[d : d + 1, :], slot.shape))
                for d in range(parity, n_col, 2)
            ],
            axis=0,
        )
        taken.append(dot_nt(pick, packed))
    for first in range(0, chips, share):
        for parity in range(2):
            mixed = taken[parity][first * SLOTS : (first + 1) * SLOTS]
            for j in range(1, share):
                rows = slice((first + j) * SLOTS, (first + j + 1) * SLOTS)
                mixed = jnp.where(lane16 >= 16 * j, taken[parity][rows], mixed)
            turned = jnp.concatenate([mixed, pad], axis=0).T
            for j in range(share):
                d = 2 * (first + j) + parity
                block = turned[16 * j : 16 * j + 8] + turned[16 * j + 8 : 16 * j + 16]
                block = pltpu.roll(block, core * (LANES - SLOTS), 1)
                block = jnp.where(line == ROWS, count[d : d + 1, :], block)
                lists[parity, first + j] = block[0 : ROWS + 1]

    loads[2].wait()
    loads[3].wait()
    bins = cbin[...]
    bin_row = (bins // tile_c).astype(F32)
    bin_col = (bins % tile_c).astype(F32)
    by_lane = jnp.zeros((tile_c, LANES), F32)
    sub = iota((tile_c, LANES), 0)
    for j in range(cells // LANES):
        part = slice(j * LANES, (j + 1) * LANES)
        by_lane = by_lane + jnp.where(sub == bin_col[:, part], area[:, part], 0.0)
    early_s[...] = jnp.sum(by_lane.T, axis=0, keepdims=True)

    pl.semaphore_wait(barrier, chips + n_row - 1)
    swap = pltpu.make_async_remote_copy(
        src_ref=lists.at[1 - core], dst_ref=swapped, send_sem=swap_sem.at[0],
        recv_sem=swap_sem.at[1], device_id=partner, device_id_type=MESH,
    )
    swap.start()
    push(early_s, early_r.at[row], early_sem, row_peers)
    early_r[row] = early_s[...]
    swap.wait_recv()
    for p in range(chips):
        send[p] = (lists[core, p] + swapped[p])[0:ROWS]
    for o, peer in chip_peers:
        pltpu.make_async_remote_copy(
            src_ref=send.at[peer], dst_ref=recv.at[chip],
            send_sem=net_sent, recv_sem=net_got.at[group_of[o]],
            device_id={"col": 2 * peer + core}, device_id_type=MESH,
        ).start()
    recv[chip] = send[chip]
    over = jnp.zeros((1, LANES), F32)
    for p in range(chips):
        ours, theirs = lists[core, p][ROWS:], swapped[p][ROWS:]
        spilt = (ours > SLOTS) | (theirs > SLOTS) | (ours + theirs > LANES)
        over = over + jnp.where(spilt, 1.0, 0.0)
    spill[...] = over

    await_bytes(early_r, n_row - 1, early_sem.at[0])
    for h in range(tile_r // 256):
        onehot[h * 256 : (h + 1) * 256, :] = ones_where(
            iota((256, cells), 0, BF16)
            == jnp.broadcast_to((bin_row - 256.0 * h).astype(BF16), (256, cells))
        )
    in_col = iota((tile_c, cells), 0, BF16) == jnp.broadcast_to(bin_col.astype(BF16), (tile_c, cells))
    area_hi, area_lo = split2(area[...])
    nought = jnp.zeros((), BF16)
    by_col = jnp.concatenate(
        [
            jnp.where(in_col, jnp.broadcast_to(area_hi, (tile_c, cells)), nought),
            jnp.where(in_col, jnp.broadcast_to(area_lo, (tile_c, cells)), nought),
        ],
        axis=0,
    )
    bin_area = dot_nt(onehot[...], by_col)
    bin_area = bin_area[:, :tile_c] + bin_area[:, tile_c:]
    w_hi, w_lo = split2(bin_area)
    upper = ones_where(iota((tile_r, tile_r), 0) <= iota((tile_r, tile_r), 1))
    below = dot(upper, jnp.concatenate([w_hi, w_lo], axis=1))
    fall[...] = below[:, :tile_c] + below[:, tile_c:]

    loads[4].wait()
    shift = (col * tile_c).astype(F32)
    for g, group in enumerate(groups):
        if g == len(groups) - 1:
            await_bytes(early_r, n_row - 1, early_sem.at[1])
            areas_below = jnp.zeros((1, tile_c), F32)
            for r in range(n_row):
                areas_below = areas_below + jnp.where(r > row, early_r[r], 0.0)
            kept[...] = areas_below
        await_bytes(recv, len(group) - (1 if g == 0 else 0), net_got.at[g])
        merged = [recv[lax.rem(chip + o, chips)] for o in group]
        merged = jnp.concatenate(merged, axis=1)
        total = merged.shape[1]
        full = lambda x, n: jnp.broadcast_to(x, (n, total))
        x_lo = jnp.clip(merged[0:1] - shift, 0.0, 1.0 * tile_c).astype(BF16)
        x_hi = jnp.clip(merged[1:2] - shift, 0.0, 1.0 * tile_c).astype(BF16)
        at = iota((tile_c, total), 0, BF16)
        col_weight = jnp.where(
            (at >= full(x_lo, tile_c)) & (at < full(x_hi, tile_c)),
            full(merged[4:5].astype(BF16), tile_c), nought,
        )
        at = iota((256, total), 0, BF16)
        for h in range(tile_r // 256):
            y_lo = jnp.clip(merged[2:3] - 256.0 * h, 0.0, 256.0).astype(BF16)
            y_hi = jnp.clip(merged[3:4] - 256.0 * h, 0.0, 256.0).astype(BF16)
            row_hit = ones_where((at >= full(y_lo, 256)) & (at < full(y_hi, 256)))
            part = dot_nt(row_hit, col_weight)
            rows = slice(h * 256, (h + 1) * 256)
            rudy[rows, :] = part if g == 0 else rudy[rows, :] + part

    excess = jnp.maximum(rudy[...] - cap[...], 0.0)
    column = jnp.sum(excess, axis=0, keepdims=True)
    mid_s[0:1, :] = column
    mid_s[1:2, :] = (
        jnp.sum(excess * fall[...], axis=0, keepdims=True) + column * kept[...]
        + 1e30 * spill[...]
    )
    mid_s[2:3, :] = early_s[...]
    push(mid_s, mid_r.at[member], mid_sem, plane)
    mid_r[member] = mid_s[...]
    swap.wait_send()
    e_hi, e_lo = split2(jnp.maximum(rudy[...] - cap[...], 0.0))
    lower = ones_where(iota((tile_r, tile_r), 0) >= iota((tile_r, tile_r), 1))
    within = dot(lower, jnp.concatenate([e_hi, e_lo], axis=1))
    infl[...] = within[:, :tile_c] + within[:, tile_c:]
    await_bytes(mid_r, 4 * n_row - 1, mid_sem.at[1])
    parts = [mid_r[m] for m in range(4 * n_row)]
    while len(parts) > 1:
        parts = [a + b for a, b in zip(parts[::2], parts[1::2])]
    factor = 2.0 / (tile_r * n_row)
    fin_s[0:1, :] = parts[0][2:3] + factor * parts[0][1:2]
    fin_s[1:2, :] = parts[0][2:3]
    quads = n_col // 4
    push(
        fin_s, fin_r.at[quad], fin_sem,
        [
            {"col": 4 * lax.rem(quad + dz, quads) + place4}
            for dz in sorted(range(1, quads), key=lambda d: -min(d, quads - d))
        ],
    )
    fin_r[quad] = fin_s[...]
    carried = jnp.zeros((1, tile_c), F32)
    for r in range(n_row):
        carried = carried + jnp.where(r < row, mid_r[4 * r + place4][0:1], 0.0)

    inflation = 1.0 + factor * (infl[...] + carried)
    infl[...] = inflation
    i_hi, i_lo = split2(inflation.T)
    looked = dot(jnp.concatenate([i_hi, i_lo], axis=0), onehot[...])
    looked = looked[:tile_c] + looked[tile_c:]
    in_col = iota((tile_c, cells), 0) == jnp.broadcast_to(bin_col, (tile_c, cells))
    looked = jnp.sum(jnp.where(in_col, looked, 0.0), axis=0, keepdims=True)
    grown[...] = area[...] * looked

    await_bytes(send, chips - 1, net_sent)
    await_bytes(mid_r, 4 * n_row - 1, mid_sem.at[0])
    await_bytes(fin_r, quads - 1, fin_sem.at[1])
    parts = [fin_r[c] for c in range(quads)]
    while len(parts) > 1:
        parts = [a + b for a, b in zip(parts[::2], parts[1::2])]
    totals[...] = parts[0]
    await_bytes(fin_r, quads - 1, fin_sem.at[0])


def finish_kernel(rudy, infl, grown, totals, rudy_h, infl_h, sizes_h, flag_h, sizes, flag, sem):
    rows = rudy.shape[0] // PIECES
    stores = []
    for src, dst, done in ((rudy, rudy_h, sem.at[0]), (infl, infl_h, sem.at[1])):
        for i in range(PIECES):
            piece = pl.ds(i * rows, rows)
            pltpu.make_async_copy(src.at[piece], dst.at[piece], done).start()
        stores.append(pltpu.make_async_copy(src, dst, done))
    stores.append(pltpu.make_async_copy(sizes, sizes_h, sem.at[2]))
    stores.append(pltpu.make_async_copy(flag, flag_h, sem.at[3]))
    sums = jnp.sum(totals[...], axis=1, keepdims=True)
    flag[...] = jnp.broadcast_to(sums[0:1], flag.shape)
    stores[3].start()
    sizes[...] = grown[...] * (sums[1:2] / sums[0:1])
    stores[2].start()
    for store in stores:
        store.wait()


def sparse_program(n_row, n_col, boxes, pins, capacity, cell_bin, cell_area):
    tile_r, tile_c = capacity.shape
    nets = pins.shape[0]
    cells = cell_bin.shape[1]
    vm = pltpu.VMEM
    dma = pltpu.SemaphoreType.DMA
    anywhere = pl.BlockSpec(memory_space=pl.ANY)
    inside = pl.BlockSpec(memory_space=pltpu.VMEM)
    shape = jax.ShapeDtypeStruct
    held = pl.pallas_call(
        functools.partial(sparse_kernel, n_row, n_col),
        name="nets_to_tiles",
        out_shape=(
            vm((tile_r, tile_c), F32), vm((tile_r, tile_c), F32),
            vm((1, cells), F32), vm((2, LANES), F32),
        ),
        in_specs=[anywhere] * 5,
        out_specs=(inside,) * 4,
        scratch_shapes=[
            vm((4, nets), jnp.int32), vm((1, nets), jnp.int32), vm((tile_r, tile_c), F32),
            vm((1, cells), jnp.int32), vm((1, cells), F32),
            vm((16, nets), F32), vm((nets // LANES, LANES), F32),
            vm((2 * HALF_SLOTS, 2 * HALF_SLOTS + LANES), BF16),
            vm((2, n_col // 2, ROWS + 1, LANES), F32), vm((n_col // 2, ROWS + 1, LANES), F32),
            vm((n_col // 2, ROWS, LANES), F32), vm((n_col // 2, ROWS, LANES), F32),
            vm((1, LANES), F32),
            vm((tile_r, cells), BF16),
            vm((1, tile_c), F32), vm((n_row, 1, tile_c), F32),
            vm((3, tile_c), F32), vm((4 * n_row, 3, tile_c), F32),
            vm((2, tile_c), F32), vm((n_col // 4, 2, tile_c), F32),
            vm((tile_r, tile_c), F32), vm((1, tile_c), F32),
            dma((5,)), dma((2,)), dma(()), dma((4,)), dma((2,)), dma((2,)), dma((2,)),
        ],
        compiler_params=pltpu.CompilerParams(
            collective_id=0, has_side_effects=True, vmem_limit_bytes=24 * 1024 * 1024
        ),
    )(boxes, pins.reshape(1, nets), capacity, cell_bin, cell_area)
    return pl.pallas_call(
        finish_kernel,
        name="finish",
        out_shape=(
            shape((tile_r, tile_c), F32), shape((tile_r, tile_c), F32), shape((1, cells), F32),
            shape((1, LANES), F32),
        ),
        in_specs=[inside] * 4,
        out_specs=(anywhere,) * 4,
        scratch_shapes=[vm((1, cells), F32), vm((1, LANES), F32), dma((4,))],
        compiler_params=pltpu.CompilerParams(vmem_limit_bytes=4 * 1024 * 1024),
    )(*held)


def to_everyone(shard, axis):
    peers = lax.axis_size(axis)
    return lax.all_to_all(
        jnp.broadcast_to(shard[None], (peers, *shard.shape)), axis, 0, 0, tiled=True
    )


def dense_program(boxes, pins, capacity, cell_bin, cell_area):
    tile_rows, tile_cols = capacity.shape
    table = jnp.concatenate([boxes, pins[None, :]], axis=0)
    table = to_everyone(table, "col")
    rows_here = lax.axis_index("row") * tile_rows + jnp.arange(tile_rows, dtype=jnp.int32)
    cols_here = lax.axis_index("col") * tile_cols + jnp.arange(tile_cols, dtype=jnp.int32)

    def add_block(index, acc):
        first_x, last_x, first_y, last_y, pin = table[index]
        span_x = (last_x - first_x + 1).astype(F32)
        span_y = (last_y - first_y + 1).astype(F32)
        weight = jnp.log(pin.astype(F32)) * (span_x + span_y) / (span_x * span_y)
        row_hits = (rows_here[:, None] >= first_y[None, :]) & (rows_here[:, None] <= last_y[None, :])
        col_hits = (cols_here[:, None] >= first_x[None, :]) & (cols_here[:, None] <= last_x[None, :])
        weighted = jnp.where(col_hits, weight.astype(BF16)[None, :], jnp.zeros((), BF16))
        return acc + dot_nt(row_hits.astype(BF16), weighted)

    rudy = lax.fori_loop(
        0, table.shape[0], add_block, jnp.zeros((tile_rows, tile_cols), F32)
    )
    excess = jnp.maximum(rudy - capacity, 0.0)
    ladder = jnp.arange(tile_rows, dtype=jnp.int32)
    lower = (ladder[:, None] >= ladder[None, :]).astype(F32)
    within = jnp.dot(
        lower, excess, precision=lax.Precision.HIGHEST, preferred_element_type=F32
    )
    sums = to_everyone(within[-1][None, :], "row")[:, 0]
    above = jnp.arange(sums.shape[0], dtype=jnp.int32) < lax.axis_index("row")
    carried = jnp.sum(jnp.where(above[:, None], sums, 0.0), axis=0)
    inflation = 1.0 + 2.0 * (within + carried[None, :]) / (tile_rows * lax.axis_size("row"))
    looked = jnp.take(inflation.reshape(-1), cell_bin[0], axis=0)
    grown = cell_area * looked[None, :]
    totals = jnp.stack([jnp.sum(cell_area), jnp.sum(grown)])[None, :]
    for axis in ("row", "col"):
        totals = jnp.sum(to_everyone(totals, axis), axis=0)
    cell_sizes = grown * (totals[0, 0] / totals[0, 1])
    return rudy, inflation, cell_sizes


def per_device(n_row, n_col, *args):
    rudy, inflation, cell_sizes, flag = sparse_program(n_row, n_col, *args)

    def again(state):
        held = [jnp.where(state[3][0, 0] > 1e20, x, jnp.ones((), x.dtype)) for x in args]
        return (*dense_program(*held), jnp.zeros_like(flag))

    state = lax.while_loop(
        lambda state: state[3][0, 0] > 1e20, again, (rudy, inflation, cell_sizes, flag)
    )
    return state[:3]


def solution(mesh):
    n_row, n_col = mesh.shape["row"], mesh.shape["col"]
    placed = (P(None, "col"), P("col"), P("row", "col"), P("row", "col"), P("row", "col"))
    return jax.shard_map(
        functools.partial(per_device, n_row, n_col),
        mesh=mesh,
        in_specs=placed,
        out_specs=(P("row", "col"),) * 3,
        check_vma=False,
    )
```
